32 devices in a mesh: seq: 8 (over z, y), dp: 4 (over x, core).
Axes of the slice: x: 2, y: 2, z: 4, core: 2. Of those that a mesh axis runs over, the one named last changes fastest.
Arguments:
- attention_queries: bfloat16 [8, 2, 256, 4096], P('seq', None, 'dp'), parts along dimension 2, may hold values from -5.5 to 5.5
- attention_keys: bfloat16 [8, 2, 256, 512], P('seq', None, 'dp'), parts along dimension 2, may hold values from -7.5 to 7.5
- attention_values: bfloat16 [8, 2, 256, 512], P('seq', None, 'dp'), parts along dimension 2, may hold values from -6 to 6
- attention_output: bfloat16 [8, 2, 256, 4096], P('seq', None, 'dp'), parts along dimension 2, may hold values from -6 to 6
- output_gradient: bfloat16 [8, 2, 256, 4096], P('seq', None, 'dp'), parts along dimension 2, may hold values from -48 to 48
- logsumexp_rows: float32 [8, 2, 256, 32], P('seq', None, 'dp'), parts along dimension 2, as said below
Outputs:
- grad_query: float32 [8, 2, 256, 4096], P('seq', None, 'dp'), parts along dimension 2
- key_gradient: float32 [8, 2, 256, 512], P('seq', None, 'dp'), parts along dimension 2
- value_gradient: float32 [8, 2, 256, 512], P('seq', None, 'dp'), parts along dimension 2
The draws below stay inside these ranges and needn't reach their ends.
There are 4 independent parts, one for each index of `dp`. The reference program is written for one: setup_inputs(seed, part) draws one part's arguments, and reference() takes and returns one part's arrays. A program takes and returns all parts, laid end to end along the dimension named above; each array names one. Nothing has to cross between parts.
Inputs may be any that keep to these rules, and one draw needn't show every extreme that they name: logsumexp_rows[i, h] is the logarithm of the sum over key positions t <= i of exp(scores[h, i, t]), computed from attention_queries and attention_keys in float32.
All inputs are finite; a program needn't handle non-finite values.
Results may differ from the reference program's by a relative error of at most 0.0003.
Values may be sent and summed in bfloat16 or wider, within the bound.
A program may use at most 128 MiB of HBM per device.

```python
import jax
import jax.numpy as jnp
from jax import lax

HQ = 32
KEY_VALUE_HEADS = 4
HEAD_SIZE = 128
QUERY_PER_KV = 8
BLOCK_TOKENS = 64
BLOCK_PAIRS = 8


def draw_attention_queries(key, part):
    complete_shape = (BLOCK_PAIRS, 2, BLOCK_TOKENS, HQ * HEAD_SIZE)
    sampled_inputs = jnp.clip(jax.random.normal(jax.random.fold_in(key, 11), complete_shape, jnp.float32), -4.0, 4.0)
    return sampled_inputs.astype(jnp.bfloat16)


def draw_attention_keys(key, part):
    complete_shape = (BLOCK_PAIRS, 2, BLOCK_TOKENS, KEY_VALUE_HEADS, HEAD_SIZE)
    sampled_inputs = jnp.clip(jax.random.normal(jax.random.fold_in(key, 13), complete_shape, jnp.float32), -4.0, 4.0)
    sampled_inputs = sampled_inputs.reshape(BLOCK_PAIRS, 2, BLOCK_TOKENS, KEY_VALUE_HEADS * HEAD_SIZE)
    return sampled_inputs.astype(jnp.bfloat16)


def sequence_row_list(blocks):
    width = blocks.shape[-1]
    earlier_half = blocks[:, 0].reshape(BLOCK_PAIRS * BLOCK_TOKENS, width)
    later_half = blocks[::-1, 1].reshape(BLOCK_PAIRS * BLOCK_TOKENS, width)
    return jnp.concatenate([earlier_half, later_half], axis=0)


def draw_logsumexp_rows(key, part):
    sequence_length = 2 * BLOCK_PAIRS * BLOCK_TOKENS
    span_rows = 2 * BLOCK_TOKENS
    query_values_list = sequence_row_list(draw_attention_queries(key, part).astype(jnp.float32)).reshape(sequence_length, KEY_VALUE_HEADS, QUERY_PER_KV, HEAD_SIZE)
    every_key = sequence_row_list(draw_attention_keys(key, part).astype(jnp.float32)).reshape(sequence_length, KEY_VALUE_HEADS, HEAD_SIZE)
    key_pos = jnp.arange(sequence_length, dtype=jnp.int32)

    def per_block(block_index):
        first_row = (block_index * span_rows).astype(jnp.int32)
        query_blk = lax.dynamic_slice_in_dim(query_values_list, first_row, span_rows, 0)
        query_pos = first_row + jnp.arange(span_rows, dtype=jnp.int32)
        allowed = key_pos[None, :] <= query_pos[:, None]
        scores = HEAD_SIZE ** (-0.5) * jnp.einsum('qhgd,khd->hgqk', query_blk, every_key, precision=lax.Precision.HIGHEST)
        largest = jnp.max(jnp.where(allowed, scores, -1e+30), axis=-1, keepdims=True)
        expsum = jnp.sum(jnp.where(allowed, jnp.exp(scores - largest), 0.0), axis=-1, keepdims=True)
        totals = (largest + jnp.log(expsum))[..., 0]
        return totals.transpose(2, 0, 1).reshape(span_rows, HQ)
    rows_all = lax.map(per_block, jnp.arange(BLOCK_PAIRS, dtype=jnp.int32)).reshape(sequence_length, HQ)
    earlier_half = rows_all[:BLOCK_PAIRS * BLOCK_TOKENS].reshape(BLOCK_PAIRS, BLOCK_TOKENS, HQ)
    later_half = rows_all[BLOCK_PAIRS * BLOCK_TOKENS:].reshape(BLOCK_PAIRS, BLOCK_TOKENS, HQ)[::-1]
    return jnp.stack([earlier_half, later_half], axis=1).astype(jnp.float32)


def shard_levels(key, extent, cuts, least, high):
    gain = 1.0
    for position, shards_of in cuts:
        draws = jax.random.uniform(jax.random.fold_in(jax.random.fold_in(key, 6), position), (shards_of,), jnp.float32, least / len(cuts), high / len(cuts))
        gain = gain * jnp.repeat(jnp.exp(draws), extent[position] // shards_of).reshape((-1,) + (1,) * (len(extent) - 1 - position))
    return gain


def gaussian(key, extent, deviation, bound, cuts=(), held_as=jnp.bfloat16):
    values = jax.random.normal(key, extent, jnp.float32) * deviation
    if len(cuts) > 0:
        values = shard_levels(key, extent, cuts, -0.22, 0.18) * values
    return jnp.clip(values, min=-bound, max=bound).astype(held_as)


def setup_inputs(seed: int = 0, part: int = 0) -> dict:
    streams_of = jax.random.split(jax.random.key(seed), 7)
    part_splits = jax.random.split(jax.random.fold_in(streams_of[6], part), 7)
    return {
        "attention_queries": draw_attention_queries(jax.random.fold_in(jax.random.fold_in(streams_of[6], part), 71), part),
        "attention_keys": draw_attention_keys(jax.random.fold_in(jax.random.fold_in(streams_of[6], part), 71), part),
        "attention_values": gaussian(part_splits[2], (BLOCK_PAIRS, 2, BLOCK_TOKENS, KEY_VALUE_HEADS * HEAD_SIZE), 1.0, 6.0, ((0, 8),)),
        "attention_output": gaussian(part_splits[3], (BLOCK_PAIRS, 2, BLOCK_TOKENS, HQ * HEAD_SIZE), 1.0, 6.0, ((0, 8),)),
        "output_gradient": gaussian(part_splits[4], (BLOCK_PAIRS, 2, BLOCK_TOKENS, HQ * HEAD_SIZE), 8.0, 48.0, ((0, 8),)),
        "logsumexp_rows": draw_logsumexp_rows(jax.random.fold_in(jax.random.fold_in(streams_of[6], part), 71), part),
    }


def blocks_to_sequence(blocks):
    earlier_half = blocks[:, 0].reshape(BLOCK_PAIRS * BLOCK_TOKENS, blocks.shape[-1])
    later_half = blocks[::-1, 1].reshape(BLOCK_PAIRS * BLOCK_TOKENS, blocks.shape[-1])
    return jnp.concatenate([earlier_half, later_half], axis=0)


def to_blocks(sequence):
    earlier_half = sequence[: BLOCK_PAIRS * BLOCK_TOKENS].reshape(BLOCK_PAIRS, BLOCK_TOKENS, sequence.shape[-1])
    later_half = sequence[BLOCK_PAIRS * BLOCK_TOKENS:].reshape(BLOCK_PAIRS, BLOCK_TOKENS, sequence.shape[-1])[::-1]
    return jnp.stack([earlier_half, later_half], axis=1)


def split_low(values):
    high_part = values.astype(jnp.bfloat16)
    back_value = lax.optimization_barrier(high_part).astype(jnp.float32)
    rest_part = (values - back_value).astype(jnp.bfloat16)
    return high_part.astype(jnp.float32), rest_part.astype(jnp.float32)


def reference(attention_queries, attention_keys, attention_values, attention_output, output_gradient, logsumexp_rows):
    scaling = HEAD_SIZE ** -0.5
    sequence_length = 2 * BLOCK_PAIRS * BLOCK_TOKENS
    span_rows = 2 * BLOCK_TOKENS
    query_values_list = blocks_to_sequence(attention_queries).reshape(sequence_length, KEY_VALUE_HEADS, QUERY_PER_KV, HEAD_SIZE)
    gradient_sequence = blocks_to_sequence(output_gradient).reshape(sequence_length, KEY_VALUE_HEADS, QUERY_PER_KV, HEAD_SIZE)
    output_sequence = blocks_to_sequence(attention_output).reshape(sequence_length, KEY_VALUE_HEADS, QUERY_PER_KV, HEAD_SIZE)
    logsum_sequence = blocks_to_sequence(logsumexp_rows).reshape(sequence_length, KEY_VALUE_HEADS, QUERY_PER_KV)
    key_as_float = blocks_to_sequence(attention_keys).reshape(sequence_length, KEY_VALUE_HEADS, HEAD_SIZE).astype(jnp.float32)
    value_as_float = blocks_to_sequence(attention_values).reshape(sequence_length, KEY_VALUE_HEADS, HEAD_SIZE).astype(jnp.float32)
    key_pos = jnp.arange(sequence_length, dtype=jnp.int32)

    def per_block(carried, block_index):
        grad_keys, grad_values = carried
        first_row = (block_index * span_rows).astype(jnp.int32)
        query_blk = lax.dynamic_slice_in_dim(query_values_list, first_row, span_rows, 0).astype(jnp.float32)
        grad_blk = lax.dynamic_slice_in_dim(gradient_sequence, first_row, span_rows, 0).astype(jnp.float32)
        output_blk = lax.dynamic_slice_in_dim(output_sequence, first_row, span_rows, 0).astype(jnp.float32)
        log_blk = lax.dynamic_slice_in_dim(logsum_sequence, first_row, span_rows, 0).transpose(1, 2, 0)[..., None]
        query_pos = first_row + jnp.arange(span_rows, dtype=jnp.int32)
        allowed = key_pos[None, :] <= query_pos[:, None]
        scores = scaling * jnp.einsum("qhgd,khd->hgqk", query_blk, key_as_float)
        weights = jnp.where(allowed, jnp.exp(scores - log_blk), 0.0)
        weights_high, weights_rest = split_low(weights)
        row_delta = jnp.sum(grad_blk * output_blk, axis=-1)
        weight_grad = jnp.einsum("qhgd,khd->hgqk", grad_blk, value_as_float)
        score_grad = weights * (weight_grad - row_delta.transpose(1, 2, 0)[..., None])
        score_high, score_rest = split_low(score_grad)
        grad_values = grad_values + jnp.einsum("hgqk,qhgd->khd", weights_high, grad_blk) + jnp.einsum("hgqk,qhgd->khd", weights_rest, grad_blk)
        grad_keys = grad_keys + scaling * (jnp.einsum("hgqk,qhgd->khd", score_high, query_blk) + jnp.einsum("hgqk,qhgd->khd", score_rest, query_blk))
        grad_query = scaling * (jnp.einsum("hgqk,khd->qhgd", score_high, key_as_float) + jnp.einsum("hgqk,khd->qhgd", score_rest, key_as_float))
        return (grad_keys, grad_values), grad_query

    zero_key_value = jnp.zeros((sequence_length, KEY_VALUE_HEADS, HEAD_SIZE), jnp.float32)
    final_results, grad_blocks = lax.scan(per_block, (zero_key_value, zero_key_value), jnp.arange(BLOCK_PAIRS, dtype=jnp.int32))
    grad_query = grad_blocks.reshape(sequence_length, HQ * HEAD_SIZE)
    key_gradient = final_results[0].reshape(sequence_length, KEY_VALUE_HEADS * HEAD_SIZE)
    value_gradient = final_results[1].reshape(sequence_length, KEY_VALUE_HEADS * HEAD_SIZE)
    return to_blocks(grad_query), to_blocks(key_gradient), to_blocks(value_gradient)
```

```python
import functools

import jax
import jax.numpy as jnp
from jax import lax
from jax.experimental import pallas as pl
from jax.experimental.pallas import tpu as pltpu
from jax.sharding import PartitionSpec as P

HEAD_SIZE = 128
LOG2E = 1.4426950408889634
LN2 = 0.6931471805599453
SPAN = 240.0
MESH = pl.DeviceIdType.MESH
KEYS, VALUES = 0, 1
RIGHT, LEFT = 0, 1


def ring_place(index, size):
    return jnp.where(index % 2 == 0, index // 2, size - 1 - index // 2)


def ring_index(place, size):
    return jnp.where(place < size // 2, 2 * place, 2 * (size - 1 - place) + 1)


def split_parts(values):
    high = values.astype(jnp.bfloat16)
    rest = (values - high.astype(jnp.float32)).astype(jnp.bfloat16)
    return jnp.concatenate([high, rest], axis=0)


def dot(a, b):
    return jnp.dot(a, b, preferred_element_type=jnp.float32)


def encode(values):
    scale = jnp.maximum(jnp.max(jnp.abs(values), axis=0, keepdims=True), 1e-30)
    level = values * (SPAN / scale)
    code = jnp.exp2(jnp.abs(level) - 0.5 * SPAN)
    return jnp.where(level < 0.0, -code, code).astype(jnp.bfloat16), scale


def decode(code, scale):
    code = code.astype(jnp.float32)
    size = jnp.log(jnp.abs(code)) * (scale * (1.0 / (SPAN * LN2))) + 0.5 * scale
    return jnp.where(code < 0.0, -size, size)


def kernel(
    n,
    q_ref,
    k_ref,
    v_ref,
    o_ref,
    g_ref,
    lse_ref,
    gq_ref,
    gk_ref,
    gv_ref,
    qs,
    gs,
    qt,
    gt,
    delta,
    dqt,
    kv,
    part,
    coded,
    scales,
    landed,
    landed_scales,
    ag_send,
    ag_recv,
    rs_send,
    rs_recv,
):
    half = n // 2
    rows = k_ref.shape[2]
    kv_heads = k_ref.shape[3] // HEAD_SIZE
    group = q_ref.shape[3] // k_ref.shape[3]
    wide = group * rows
    scaling = HEAD_SIZE ** (-0.5)
    me = lax.axis_index("seq")
    place = ring_place(me, n)
    right = ring_index(lax.rem(place + 1, n), n)
    left = ring_index(lax.rem(place + n - 1, n), n)
    target = (right, left)

    barrier = pltpu.get_barrier_semaphore()
    for neighbour in (left, right):
        pl.semaphore_signal(barrier, inc=1, device_id={"seq": neighbour}, device_id_type=MESH)
    pl.semaphore_wait(barrier, 2)

    def gather_copy(way, what, distance, own):
        arrives = n - distance if way == RIGHT else distance
        held = lax.rem(n + 1 - distance, n) if way == RIGHT else distance - 1
        source = (k_ref, v_ref)[what].at[0] if own else kv.at[held, what]
        return pltpu.make_async_remote_copy(
            src_ref=source,
            dst_ref=kv.at[arrives, what],
            send_sem=ag_send.at[way, distance - 1, what],
            recv_sem=ag_recv.at[way, distance - 1, what],
            device_id={"seq": target[way]},
            device_id_type=MESH,
        )

    def sum_copies(what, step, block):
        return [
            pltpu.make_async_remote_copy(
                src_ref=source.at[what, step, block],
                dst_ref=sink.at[what, step, block],
                send_sem=rs_send.at[what, step, block, i],
                recv_sem=rs_recv.at[what, step, block, i],
                device_id={"seq": target[what]},
                device_id_type=MESH,
            )
            for i, (source, sink) in enumerate(((coded, landed), (scales, landed_scales)))
        ]

    for what in (KEYS, VALUES):
        for way in (RIGHT, LEFT):
            if half > 1 or what == way:
                gather_copy(way, what, 1, True).start()

    def prepare(g, _):
        for a in range(2):
            products = []
            for j in range(group):
                columns = pl.ds(pl.multiple_of((g * group + j) * HEAD_SIZE, HEAD_SIZE), HEAD_SIZE)
                grad = g_ref[0, a, :, columns]
                qs[g, a, pl.ds(j * rows, rows), :] = q_ref[0, a, :, columns]
                gs[g, a, pl.ds(j * rows, rows), :] = grad
                products.append(grad.astype(jnp.float32) * o_ref[0, a, :, columns].astype(jnp.float32))
            turned = jnp.transpose(jnp.concatenate(products, axis=0))
            delta[g, a] = jnp.sum(turned, axis=0, keepdims=True)
            qt[g, a] = jnp.transpose(qs[g, a])
            gt[g, a] = jnp.transpose(gs[g, a])
        return 0

    lax.fori_loop(0, kv_heads, prepare, 0)

    def unit(keys, values, g, a, mask=None):
        count = keys.shape[0]
        scores = dot(keys, qt[g, a])
        weights = jnp.exp2(scores * (scaling * LOG2E) - lse_ref[g, a])
        if mask is not None:
            weights = jnp.where(mask, weights, 0.0)
        value_part = dot(split_parts(weights), gs[g, a])
        score_grad = weights * (dot(values, gt[g, a]) - delta[g, a])
        split = split_parts(score_grad)
        key_part = dot(split, qs[g, a])
        turned = jnp.transpose(keys)
        query_part = dot(jnp.concatenate([turned, turned], axis=1), split)
        return key_part[:count] + key_part[count:], value_part[:count] + value_part[count:], query_part

    def columns_of(g):
        return pl.ds(pl.multiple_of(g * HEAD_SIZE, HEAD_SIZE), HEAD_SIZE)

    def for_heads(head):
        def one(g, _):
            head(g, columns_of(g))
            return 0

        lax.fori_loop(0, kv_heads, one, 0, unroll=UNROLL)

    def shard(slot):
        later = ring_index(lax.rem(place + slot, n), n) > me

        @pl.when(later)
        def _():
            def head(g, cols):
                keys = kv[slot, KEYS, :, :, cols].reshape(2 * rows, HEAD_SIZE)
                values = kv[slot, VALUES, :, :, cols].reshape(2 * rows, HEAD_SIZE)
                out = unit(keys, values, g, 1)
                for what in (KEYS, VALUES):
                    part[what, slot, :, :, cols] = out[what].reshape(2, rows, HEAD_SIZE)
                dqt[g, 1] += out[2]

            for_heads(head)

        @pl.when(jnp.logical_not(later))
        def _():
            def head(g, cols):
                keys = kv[slot, KEYS, 0, :, cols]
                values = kv[slot, VALUES, 0, :, cols]
                outs = [unit(keys, values, g, a) for a in range(2)]
                for what in (KEYS, VALUES):
                    part[what, slot, 0, :, cols] = outs[0][what] + outs[1][what]
                    part[what, slot, 1, :, cols] = jnp.zeros((rows, HEAD_SIZE), jnp.float32)
                for a in range(2):
                    dqt[g, a] += outs[a][2]

            for_heads(head)

    def own_shard():
        def head(g, cols):
            key_row = lax.broadcasted_iota(jnp.int32, (2 * rows, wide), 0)
            query_row = lax.broadcasted_iota(jnp.int32, (2 * rows, wide), 1) % rows
            keys = k_ref[0, :, :, cols].reshape(2 * rows, HEAD_SIZE)
            values = v_ref[0, :, :, cols].reshape(2 * rows, HEAD_SIZE)
            first = unit(keys[:rows], values[:rows], g, 0, key_row[:rows] <= query_row[:rows])
            second = unit(keys, values, g, 1, key_row <= query_row + rows)
            for what in (KEYS, VALUES):
                part[what, 0, 0, :, cols] = first[what] + second[what][:rows]
                part[what, 0, 1, :, cols] = second[what][rows:]
            dqt[g, 0] = first[2]
            dqt[g, 1] = second[2]

        for_heads(head)

    own_shard()

    def send_sums(step, first):
        for block in range(2):
            for what in (KEYS, VALUES):
                slot = n - 1 - step if what == KEYS else 1 + step
                total = part[what, slot, block]
                if not first:
                    for copy in sum_copies(what, step - 1, block):
                        copy.wait_recv()
                    total += decode(landed[what, step - 1, block], landed_scales[what, step - 1, block])
                coded[what, step, block], scales[what, step, block] = encode(total)
                for copy in sum_copies(what, step, block):
                    copy.start()

    def near(step, first):
        gather_copy(RIGHT, KEYS, step + 1, False).wait_recv()
        gather_copy(RIGHT, KEYS, step + 2, False).start()
        gather_copy(LEFT, VALUES, step + 1, False).wait_recv()
        gather_copy(LEFT, VALUES, step + 2, False).start()
        for way, what in ((RIGHT, VALUES), (LEFT, KEYS)):
            gather_copy(way, what, step + 1, False).wait_recv()

            @pl.when(step + 2 < half)
            def _():
                gather_copy(way, what, step + 2, False).start()

        def side(which, _):
            shard(jnp.where(which == 0, n - 1 - step, 1 + step))
            return 0

        lax.fori_loop(0, 2, side, 0)
        send_sums(step, first)

    if half > 1:
        near(0, True)

        def middle(step, _):
            near(step, False)
            return 0

        lax.fori_loop(1, half - 1, middle, 0)

    gather_copy(RIGHT, KEYS, half, False).wait_recv()
    gather_copy(LEFT, VALUES, half, False).wait_recv()
    shard(half)
    send_sums(half - 1, half == 1)

    for a in range(2):

        def write(g, _):
            turned = jnp.transpose(dqt[g, a]) * scaling
            for j in range(group):
                columns = pl.ds(pl.multiple_of((g * group + j) * HEAD_SIZE, HEAD_SIZE), HEAD_SIZE)
                gq_ref[0, a, :, columns] = turned[j * rows : (j + 1) * rows]
            return 0

        lax.fori_loop(0, kv_heads, write, 0)

    def far(step, _):
        send_sums(step, False)
        return 0

    lax.fori_loop(half, n - 1, far, 0)
    for block in range(2):
        for what in (KEYS, VALUES):
            for copy in sum_copies(what, n - 2, block):
                copy.wait_recv()
            total = part[what, 0, block] + decode(landed[what, n - 2, block], landed_scales[what, n - 2, block])
            if what == KEYS:
                gk_ref[0, block] = total * scaling
            else:
                gv_ref[0, block] = total

    def sent(step, _):
        for block in range(2):
            for what in (KEYS, VALUES):
                for copy in sum_copies(what, step, block):
                    copy.wait_send()
        return 0

    lax.fori_loop(0, n - 1, sent, 0)

    def passed(distance, _):
        gather_copy(RIGHT, KEYS, distance, False).wait_send()
        gather_copy(LEFT, VALUES, distance, False).wait_send()
        gather_copy(RIGHT, VALUES, distance, False).wait_send()
        gather_copy(LEFT, KEYS, distance, False).wait_send()
        return 0

    lax.fori_loop(1, half, passed, 0)
    gather_copy(RIGHT, KEYS, half, False).wait_send()
    gather_copy(LEFT, VALUES, half, False).wait_send()


UNROLL = True


def body(queries, keys, values, output, gradient, logsumexp):
    n = lax.axis_size("seq")
    rows = keys.shape[2]
    kv_heads = keys.shape[3] // HEAD_SIZE
    group = queries.shape[3] // keys.shape[3]
    wide = group * rows
    lse = logsumexp[0].reshape(2, rows, kv_heads, group).transpose(2, 0, 3, 1)
    lse = (lse * LOG2E).reshape(kv_heads, 2, 1, wide)
    vmem = pl.BlockSpec(memory_space=pltpu.VMEM)
    pair = (2, rows, keys.shape[3])
    scale = (2, 1, keys.shape[3])
    return pl.pallas_call(
        functools.partial(kernel, n),
        out_shape=(
            jax.ShapeDtypeStruct(queries.shape, jnp.float32),
            jax.ShapeDtypeStruct(keys.shape, jnp.float32),
            jax.ShapeDtypeStruct(values.shape, jnp.float32),
        ),
        in_specs=[vmem] * 6,
        out_specs=(vmem, vmem, vmem),
        scratch_shapes=[
            pltpu.VMEM((kv_heads, 2, wide, HEAD_SIZE), jnp.bfloat16),
            pltpu.VMEM((kv_heads, 2, wide, HEAD_SIZE), jnp.bfloat16),
            pltpu.VMEM((kv_heads, 2, HEAD_SIZE, wide), jnp.bfloat16),
            pltpu.VMEM((kv_heads, 2, HEAD_SIZE, wide), jnp.bfloat16),
            pltpu.VMEM((kv_heads, 2, 1, wide), jnp.float32),
            pltpu.VMEM((kv_heads, 2, HEAD_SIZE, wide), jnp.float32),
            pltpu.VMEM((n, 2) + pair, jnp.bfloat16),
            pltpu.VMEM((2, n) + pair, jnp.float32),
            pltpu.VMEM((2, n - 1) + pair, jnp.bfloat16),
            pltpu.VMEM((2, n - 1) + scale, jnp.float32),
            pltpu.VMEM((2, n - 1) + pair, jnp.bfloat16),
            pltpu.VMEM((2, n - 1) + scale, jnp.float32),
            pltpu.SemaphoreType.DMA((2, n // 2, 2)),
            pltpu.SemaphoreType.DMA((2, n // 2, 2)),
            pltpu.SemaphoreType.DMA((2, n - 1, 2, 2)),
            pltpu.SemaphoreType.DMA((2, n - 1, 2, 2)),
        ],
        compiler_params=pltpu.CompilerParams(
            collective_id=0, has_side_effects=True, vmem_limit_bytes=64_000_000
        ),
    )(queries, keys, values, output, gradient, lse)


def solution(mesh):
    spec = P("seq", None, "dp", None)
    return jax.shard_map(
        body, mesh=mesh, in_specs=(spec,) * 6, out_specs=(spec,) * 3, check_vma=False
    )
```

```python
import functools

import jax
import jax.numpy as jnp
from jax import lax
from jax.experimental import pallas as pl
from jax.experimental.pallas import tpu as pltpu
from jax.sharding import PartitionSpec as P

HEAD_SIZE = 128
LOG2E = 1.4426950408889634
LN2 = 0.6931471805599453
SPAN = 240.0
MESH = pl.DeviceIdType.MESH
KEYS, VALUES = 0, 1
HALVES = 2
RIGHT, LEFT = 0, 1


def ring_place(index, size):
    return jnp.where(index % 2 == 0, index // 2, size - 1 - index // 2)


def ring_index(place, size):
    return jnp.where(place < size // 2, 2 * place, 2 * (size - 1 - place) + 1)


def split_parts(values):
    high = values.astype(jnp.bfloat16)
    rest = (values - high.astype(jnp.float32)).astype(jnp.bfloat16)
    return jnp.concatenate([high, rest], axis=0)


def dot(a, b):
    return jnp.dot(a, b, preferred_element_type=jnp.float32)


def encode(values):
    scale = jnp.maximum(jnp.max(jnp.abs(values), axis=0, keepdims=True), 1e-30)
    level = values * (SPAN / scale)
    code = jnp.exp2(jnp.abs(level) - 0.5 * SPAN)
    return jnp.where(level < 0.0, -code, code).astype(jnp.bfloat16), scale


def decode(code, scale):
    code = code.astype(jnp.float32)
    size = jnp.log(jnp.abs(code)) * (scale * (1.0 / (SPAN * LN2))) + 0.5 * scale
    return jnp.where(code < 0.0, -size, size)


def kernel(
    n,
    q_hbm,
    k_hbm,
    v_hbm,
    o_hbm,
    g_hbm,
    lse_hbm,
    dqt,
    gk_ref,
    gv_ref,
    q_ref,
    o_ref,
    g_ref,
    lse_ref,
    qs,
    gs,
    qt,
    gt,
    delta,
    lse,
    kv,
    part,
    coded,
    scales,
    landed,
    landed_scales,
    load_sem,
    own_sem,
    ag_send,
    ag_recv,
    rs_send,
    rs_recv,
):
    half = n // 2
    rows = k_hbm.shape[2]
    kv_heads = k_hbm.shape[3] // HEAD_SIZE
    some = kv_heads // HALVES
    columns = some * HEAD_SIZE
    group = q_hbm.shape[3] // k_hbm.shape[3]
    wide = group * rows
    scaling = HEAD_SIZE ** (-0.5)
    me = lax.axis_index("seq")
    place = ring_place(me, n)
    right = ring_index(lax.rem(place + 1, n), n)
    left = ring_index(lax.rem(place + n - 1, n), n)
    target = (right, left)

    own = [
        pltpu.make_async_copy(
            source.at[0, :, :, pl.ds(h * columns, columns)], kv.at[0, h, what], own_sem.at[h, what]
        )
        for h in range(HALVES)
        for what, source in ((KEYS, k_hbm), (VALUES, v_hbm))
    ]
    loads = [
        pltpu.make_async_copy(source, sink, load_sem.at[i])
        for i, (source, sink) in enumerate(
            ((q_hbm, q_ref), (g_hbm, g_ref), (o_hbm, o_ref), (lse_hbm, lse_ref))
        )
    ]
    for copy in own + loads:
        copy.start()

    barrier = pltpu.get_barrier_semaphore()
    for neighbour in (left, right):
        pl.semaphore_signal(barrier, inc=1, device_id={"seq": neighbour}, device_id_type=MESH)
    pl.semaphore_wait(barrier, 2)

    def gather_copy(way, h, distance):
        arrives = n - distance if way == RIGHT else distance
        held = lax.rem(n + 1 - distance, n) if way == RIGHT else distance - 1
        return pltpu.make_async_remote_copy(
            src_ref=kv.at[held, h],
            dst_ref=kv.at[arrives, h],
            send_sem=ag_send.at[way, distance - 1, h],
            recv_sem=ag_recv.at[way, distance - 1, h],
            device_id={"seq": target[way]},
            device_id_type=MESH,
        )

    def sum_copies(way, step, what):
        return [
            pltpu.make_async_remote_copy(
                src_ref=source.at[way, step, what],
                dst_ref=sink.at[way, step, what],
                send_sem=rs_send.at[way, step, what, i],
                recv_sem=rs_recv.at[way, step, what, i],
                device_id={"seq": target[way]},
                device_id_type=MESH,
            )
            for i, (source, sink) in enumerate(((coded, landed), (scales, landed_scales)))
        ]

    for copy in own:
        copy.wait()
    for turn in range(HALVES):
        for way in (RIGHT, LEFT):
            if half > 1 or turn == 0:
                gather_copy(way, way if turn == 0 else 1 - way, 1).start()
    for copy in loads:
        copy.wait()

    def prepare(g, _):
        for a in range(2):
            products = []
            for j in range(group):
                head = pl.ds(pl.multiple_of((g * group + j) * HEAD_SIZE, HEAD_SIZE), HEAD_SIZE)
                grad = g_ref[0, a, :, head]
                qs[g, a, pl.ds(j * rows, rows), :] = q_ref[0, a, :, head]
                gs[g, a, pl.ds(j * rows, rows), :] = grad
                products.append(grad.astype(jnp.float32) * o_ref[0, a, :, head].astype(jnp.float32))
            turned = jnp.transpose(jnp.concatenate(products, axis=0))
            delta[g, a] = jnp.sum(turned, axis=0, keepdims=True)
            qt[g, a] = jnp.transpose(qs[g, a])
            gt[g, a] = jnp.transpose(gs[g, a])
            tile = lse_ref[0, a, pl.ds(pl.multiple_of(g * group, group), group), :] * LOG2E
            lse[g, a] = jnp.concatenate([tile[j : j + 1] for j in range(group)], axis=1)
        return 0

    lax.fori_loop(0, kv_heads, prepare, 0)

    def unit(keys, values, g, a, mask=None):
        count = keys.shape[0]
        scores = dot(keys, qt[g, a])
        weights = jnp.exp2(scores * (scaling * LOG2E) - lse[g, a])
        if mask is not None:
            weights = jnp.where(mask, weights, 0.0)
        value_part = dot(split_parts(weights), gs[g, a])
        score_grad = weights * (dot(values, gt[g, a]) - delta[g, a])
        split = split_parts(score_grad)
        key_part = dot(split, qs[g, a])
        turned = jnp.transpose(keys)
        query_part = dot(jnp.concatenate([turned, turned], axis=1), split)
        return key_part[:count] + key_part[count:], value_part[:count] + value_part[count:], query_part

    def later_shard(slot, h, i):
        cols = pl.ds(i * HEAD_SIZE, HEAD_SIZE)
        g = h * some + i
        keys = kv[slot, h, KEYS, :, :, cols].reshape(2 * rows, HEAD_SIZE)
        values = kv[slot, h, VALUES, :, :, cols].reshape(2 * rows, HEAD_SIZE)
        out = unit(keys, values, g, 1)
        for what in (KEYS, VALUES):
            part[slot, h, what, :, :, cols] = out[what].reshape(2, rows, HEAD_SIZE)
        dqt[g, 1] += out[2]

    def earlier_shard(slot, h, i):
        cols = pl.ds(i * HEAD_SIZE, HEAD_SIZE)
        g = h * some + i
        keys = kv[slot, h, KEYS, 0, :, cols]
        values = kv[slot, h, VALUES, 0, :, cols]
        outs = [unit(keys, values, g, a) for a in range(2)]
        for what in (KEYS, VALUES):
            part[slot, h, what, 0, :, cols] = outs[0][what] + outs[1][what]
            part[slot, h, what, 1, :, cols] = jnp.zeros((rows, HEAD_SIZE), jnp.float32)
        for a in range(2):
            dqt[g, a] += outs[a][2]

    def shard(slot, h):
        later = ring_index(lax.rem(place + slot, n), n) > me

        @pl.when(later)
        def _():
            for i in range(some):
                later_shard(slot, h, i)

        @pl.when(jnp.logical_not(later))
        def _():
            for i in range(some):
                earlier_shard(slot, h, i)

    def own_shard(h, i):
        cols = pl.ds(i * HEAD_SIZE, HEAD_SIZE)
        g = h * some + i
        key_row = lax.broadcasted_iota(jnp.int32, (2 * rows, wide), 0)
        query_row = lax.broadcasted_iota(jnp.int32, (2 * rows, wide), 1) % rows
        keys = kv[0, h, KEYS, :, :, cols].reshape(2 * rows, HEAD_SIZE)
        values = kv[0, h, VALUES, :, :, cols].reshape(2 * rows, HEAD_SIZE)
        first = unit(keys[:rows], values[:rows], g, 0, key_row[:rows] <= query_row[:rows])
        second = unit(keys, values, g, 1, key_row <= query_row + rows)
        for what in (KEYS, VALUES):
            part[0, h, what, 0, :, cols] = first[what] + second[what][:rows]
            part[0, h, what, 1, :, cols] = second[what][rows:]
        dqt[g, 0] = first[2]
        dqt[g, 1] = second[2]

    def own_half(h, _):
        for i in range(some):
            own_shard(h, i)
        return 0

    lax.fori_loop(0, HALVES, own_half, 0)

    def slot_of(way, step):
        return n - 1 - step if way == RIGHT else 1 + step

    def send_sums(way, step, first):
        for what in (KEYS, VALUES):
            if not first:
                for copy in sum_copies(way, step - 1, what):
                    copy.wait_recv()
            for block in range(2):
                total = part[slot_of(way, step), way, what, block]
                if not first:
                    total += decode(landed[way, step - 1, what, block], landed_scales[way, step - 1, what, block])
                coded[way, step, what, block], scales[way, step, what, block] = encode(total)
            for copy in sum_copies(way, step, what):
                copy.start()

    def near(step, first):
        for way in (RIGHT, LEFT):
            gather_copy(way, way, step + 1).wait_recv()
            gather_copy(way, way, step + 2).start()
        for way in (RIGHT, LEFT):
            shard(slot_of(way, step), way)
            send_sums(way, step, first)
        for way in (RIGHT, LEFT):
            gather_copy(way, 1 - way, step + 1).wait_recv()

            @pl.when(step + 2 < half)
            def _():
                gather_copy(way, 1 - way, step + 2).start()

        for way in (RIGHT, LEFT):
            shard(slot_of(way, step), 1 - way)

    if half > 1:
        near(0, True)

        def middle(step, _):
            near(step, False)
            return 0

        lax.fori_loop(1, half - 1, middle, 0)

    for way in (RIGHT, LEFT):
        gather_copy(way, way, half).wait_recv()
        shard(half, way)
        send_sums(way, half - 1, half == 1)

    def far(step, _):
        for way in (RIGHT, LEFT):
            send_sums(way, step, False)
        return 0

    lax.fori_loop(half, n - 1, far, 0)
    for way in (RIGHT, LEFT):
        cols = pl.ds(way * columns, columns)
        for what in (KEYS, VALUES):
            for copy in sum_copies(way, n - 2, what):
                copy.wait_recv()
            for block in range(2):
                total = part[0, way, what, block]
                total += decode(landed[way, n - 2, what, block], landed_scales[way, n - 2, what, block])
                if what == KEYS:
                    gk_ref[0, block, :, cols] = total * scaling
                else:
                    gv_ref[0, block, :, cols] = total

    def sent(step, _):
        for way in (RIGHT, LEFT):
            for what in (KEYS, VALUES):
                for copy in sum_copies(way, step, what):
                    copy.wait_send()
        return 0

    lax.fori_loop(0, n - 1, sent, 0)

    def passed(distance, _):
        for way in (RIGHT, LEFT):
            for h in range(HALVES):
                gather_copy(way, h, distance).wait_send()
        return 0

    lax.fori_loop(1, half, passed, 0)
    for way in (RIGHT, LEFT):
        gather_copy(way, way, half).wait_send()


def finish(dqt, gk_in, gv_in, gq_ref, gk_ref, gv_ref):
    kv_heads, _, _, wide = dqt.shape
    rows = gq_ref.shape[2]
    for g in range(kv_heads):
        for a in range(2):
            turned = jnp.transpose(dqt[g, a]) * HEAD_SIZE ** (-0.5)
            for j in range(wide // rows):
                head = pl.ds((g * (wide // rows) + j) * HEAD_SIZE, HEAD_SIZE)
                gq_ref[0, a, :, head] = turned[j * rows : (j + 1) * rows]
    gk_ref[...] = gk_in[...]
    gv_ref[...] = gv_in[...]


def body(queries, keys, values, output, gradient, logsumexp):
    n = lax.axis_size("seq")
    rows = keys.shape[2]
    kv_heads = keys.shape[3] // HEAD_SIZE
    group = queries.shape[3] // keys.shape[3]
    wide = group * rows
    lse = logsumexp.transpose(0, 1, 3, 2)
    vmem = pl.BlockSpec(memory_space=pltpu.VMEM)
    hbm = pl.BlockSpec(memory_space=pl.ANY)
    columns = keys.shape[3] // HALVES
    block = (2, 2, rows, columns)
    scale = (2, 2, 1, columns)
    bf16, f32 = jnp.bfloat16, jnp.float32
    flat = (kv_heads, 2, wide, HEAD_SIZE)
    turned = (kv_heads, 2, HEAD_SIZE, wide)
    line = (kv_heads, 2, 1, wide)
    scratch = [
        (queries.shape, bf16),
        (output.shape, bf16),
        (gradient.shape, bf16),
        (lse.shape, f32),
        (flat, bf16),
        (flat, bf16),
        (turned, bf16),
        (turned, bf16),
        (line, f32),
        (line, f32),
        ((n, HALVES) + block, bf16),
        ((n, HALVES) + block, f32),
        ((2, n - 1) + block, bf16),
        ((2, n - 1) + scale, f32),
        ((2, n - 1) + block, bf16),
        ((2, n - 1) + scale, f32),
    ]
    dqt, gk, gv = pl.pallas_call(
        functools.partial(kernel, n),
        out_shape=(
            jax.ShapeDtypeStruct(turned, f32),
            jax.ShapeDtypeStruct(keys.shape, f32),
            jax.ShapeDtypeStruct(values.shape, f32),
        ),
        in_specs=[hbm] * 6,
        out_specs=(vmem, vmem, vmem),
        scratch_shapes=[pltpu.VMEM(shape, dtype) for shape, dtype in scratch]
        + [
            pltpu.SemaphoreType.DMA((4,)),
            pltpu.SemaphoreType.DMA((HALVES, 2)),
            pltpu.SemaphoreType.DMA((2, n // 2, HALVES)),
            pltpu.SemaphoreType.DMA((2, n // 2, HALVES)),
            pltpu.SemaphoreType.DMA((2, n - 1, 2, 2)),
            pltpu.SemaphoreType.DMA((2, n - 1, 2, 2)),
        ],
        compiler_params=pltpu.CompilerParams(
            collective_id=0, has_side_effects=True, vmem_limit_bytes=64_000_000
        ),
    )(queries, keys, values, output, gradient, lse)
    return pl.pallas_call(
        finish,
        out_shape=(
            jax.ShapeDtypeStruct(queries.shape, f32),
            jax.ShapeDtypeStruct(keys.shape, f32),
            jax.ShapeDtypeStruct(values.shape, f32),
        ),
        in_specs=[vmem] * 3,
        out_specs=(vmem, vmem, vmem),
    )(dqt, gk, gv)


def solution(mesh):
    spec = P("seq", None, "dp", None)
    return jax.shard_map(
        body, mesh=mesh, in_specs=(spec,) * 6, out_specs=(spec,) * 3, check_vma=False
    )
```

```python
import functools

import jax
import jax.numpy as jnp
from jax import lax
from jax.experimental import pallas as pl
from jax.experimental.pallas import tpu as pltpu
from jax.sharding import PartitionSpec as P

HEAD_SIZE = 128
LOG2E = 1.4426950408889634
LN2 = 0.6931471805599453
SPAN = 240.0
MESH = pl.DeviceIdType.MESH
KEYS, VALUES = 0, 1
HALVES = 2
PARTS = 4
RIGHT, LEFT = 0, 1


def ring_place(index, size):
    return jnp.where(index % 2 == 0, index // 2, size - 1 - index // 2)


def ring_index(place, size):
    return jnp.where(place < size // 2, 2 * place, 2 * (size - 1 - place) + 1)


def split_parts(values):
    high = values.astype(jnp.bfloat16)
    rest = (values - high.astype(jnp.float32)).astype(jnp.bfloat16)
    return jnp.concatenate([high, rest], axis=0)


def dot(a, b):
    return jnp.dot(a, b, preferred_element_type=jnp.float32)


def encode(values):
    scale = jnp.maximum(jnp.max(jnp.abs(values), axis=0, keepdims=True), 1e-30)
    level = values * (SPAN / scale)
    code = jnp.exp2(jnp.abs(level) - 0.5 * SPAN)
    return jnp.where(level < 0.0, -code, code).astype(jnp.bfloat16), scale


def decode(code, scale):
    code = code.astype(jnp.float32)
    size = jnp.log(jnp.abs(code)) * (scale * (1.0 / (SPAN * LN2))) + 0.5 * scale
    return jnp.where(code < 0.0, -size, size)


def kernel(
    n,
    q_hbm,
    k_hbm,
    v_hbm,
    o_hbm,
    g_hbm,
    lse_hbm,
    gq_hbm,
    gk_hbm,
    gv_hbm,
    q_ref,
    o_ref,
    g_ref,
    lse_ref,
    qs,
    gs,
    qt,
    gt,
    delta,
    lse,
    dqt,
    gq_ref,
    gk_ref,
    gv_ref,
    kv,
    part,
    coded,
    scales,
    landed,
    landed_scales,
    load_sem,
    own_sem,
    out_sem,
    ag_send,
    ag_recv,
    rs_send,
    rs_recv,
):
    half = n // 2
    rows = k_hbm.shape[2]
    kv_heads = k_hbm.shape[3] // HEAD_SIZE
    some = kv_heads // HALVES
    columns = some * HEAD_SIZE
    group = q_hbm.shape[3] // k_hbm.shape[3]
    wide = group * rows
    scaling = HEAD_SIZE ** (-0.5)
    me = lax.axis_index("seq")
    place = ring_place(me, n)
    right = ring_index(lax.rem(place + 1, n), n)
    left = ring_index(lax.rem(place + n - 1, n), n)
    target = (right, left)

    own = [
        pltpu.make_async_copy(
            source.at[0, :, :, pl.ds(h * columns, columns)], kv.at[0, h, what], own_sem.at[h, what]
        )
        for h in range(HALVES)
        for what, source in ((KEYS, k_hbm), (VALUES, v_hbm))
    ]
    loads = [
        pltpu.make_async_copy(source, sink, load_sem.at[i])
        for i, (source, sink) in enumerate(
            ((q_hbm, q_ref), (g_hbm, g_ref), (o_hbm, o_ref), (lse_hbm, lse_ref))
        )
    ]
    for copy in own + loads:
        copy.start()

    barrier = pltpu.get_barrier_semaphore()
    for neighbour in (left, right):
        pl.semaphore_signal(barrier, inc=1, device_id={"seq": neighbour}, device_id_type=MESH)
    pl.semaphore_wait(barrier, 2)

    def gather_copy(way, h, distance):
        arrives = n - distance if way == RIGHT else distance
        held = lax.rem(n + 1 - distance, n) if way == RIGHT else distance - 1
        return pltpu.make_async_remote_copy(
            src_ref=kv.at[held, h],
            dst_ref=kv.at[arrives, h],
            send_sem=ag_send.at[way, distance - 1, h],
            recv_sem=ag_recv.at[way, distance - 1, h],
            device_id={"seq": target[way]},
            device_id_type=MESH,
        )

    def sum_copies(way, step, what):
        return [
            pltpu.make_async_remote_copy(
                src_ref=source.at[way, step, what],
                dst_ref=sink.at[way, step, what],
                send_sem=rs_send.at[way, step, what, i],
                recv_sem=rs_recv.at[way, step, what, i],
                device_id={"seq": target[way]},
                device_id_type=MESH,
            )
            for i, (source, sink) in enumerate(((coded, landed), (scales, landed_scales)))
        ]

    for copy in own:
        copy.wait()
    for turn in range(HALVES):
        for way in (RIGHT, LEFT):
            if half > 1 or turn == 0:
                gather_copy(way, way if turn == 0 else 1 - way, 1).start()
    for copy in loads:
        copy.wait()

    def prepare(g, _):
        for a in range(2):
            products = []
            for j in range(group):
                head = pl.ds(pl.multiple_of((g * group + j) * HEAD_SIZE, HEAD_SIZE), HEAD_SIZE)
                grad = g_ref[0, a, :, head]
                qs[g, a, pl.ds(j * rows, rows), :] = q_ref[0, a, :, head]
                gs[g, a, pl.ds(j * rows, rows), :] = grad
                products.append(grad.astype(jnp.float32) * o_ref[0, a, :, head].astype(jnp.float32))
            turned = jnp.transpose(jnp.concatenate(products, axis=0))
            delta[g, a] = jnp.sum(turned, axis=0, keepdims=True)
            qt[g, a] = jnp.transpose(qs[g, a])
            gt[g, a] = jnp.transpose(gs[g, a])
            tile = lse_ref[0, a, pl.ds(pl.multiple_of(g * group, group), group), :] * LOG2E
            lse[g, a] = jnp.concatenate([tile[j : j + 1] for j in range(group)], axis=1)
        return 0

    lax.fori_loop(0, kv_heads, prepare, 0)

    def unit(keys, values, g, a, chunk, mask=None, new=False):
        count = keys.shape[0]
        turned = jnp.transpose(keys)
        turned = jnp.concatenate([turned, turned], axis=1)
        key_part = value_part = 0.0
        for i in range(0, wide, chunk):
            lanes = slice(i, i + chunk)
            scores = dot(keys, qt[g, a, :, lanes])
            weights = jnp.exp2(scores * (scaling * LOG2E) - lse[g, a, :, lanes])
            if mask is not None:
                weights = jnp.where(mask[:, lanes], weights, 0.0)
            value_part += dot(split_parts(weights), gs[g, a, lanes, :])
            score_grad = weights * (dot(values, gt[g, a, :, lanes]) - delta[g, a, :, lanes])
            split = split_parts(score_grad)
            key_part += dot(split, qs[g, a, lanes, :])
            query_part = dot(turned, split)
            if new:
                dqt[g, a, :, lanes] = query_part
            else:
                dqt[g, a, :, lanes] += query_part
        return key_part[:count] + key_part[count:], value_part[:count] + value_part[count:]

    def later_shard(slot, h, i):
        cols = pl.ds(i * HEAD_SIZE, HEAD_SIZE)
        g = h * some + i
        keys = kv[slot, h, KEYS, :, :, cols].reshape(2 * rows, HEAD_SIZE)
        values = kv[slot, h, VALUES, :, :, cols].reshape(2 * rows, HEAD_SIZE)
        out = unit(keys, values, g, 1, wide)
        for what in (KEYS, VALUES):
            part[slot, h, what, :, :, cols] = out[what].reshape(2, rows, HEAD_SIZE)

    def earlier_shard(slot, h, i):
        cols = pl.ds(i * HEAD_SIZE, HEAD_SIZE)
        g = h * some + i
        keys = kv[slot, h, KEYS, 0, :, cols]
        values = kv[slot, h, VALUES, 0, :, cols]
        outs = [unit(keys, values, g, a, wide // 2) for a in range(2)]
        for what in (KEYS, VALUES):
            part[slot, h, what, 0, :, cols] = outs[0][what] + outs[1][what]
            part[slot, h, what, 1, :, cols] = jnp.zeros((rows, HEAD_SIZE), jnp.float32)

    def shard(slot, h):
        later = ring_index(lax.rem(place + slot, n), n) > me

        @pl.when(later)
        def _():
            for i in range(some):
                later_shard(slot, h, i)

        @pl.when(jnp.logical_not(later))
        def _():
            for i in range(some):
                earlier_shard(slot, h, i)

    def own_shard(h, i):
        cols = pl.ds(i * HEAD_SIZE, HEAD_SIZE)
        g = h * some + i
        key_row = lax.broadcasted_iota(jnp.int32, (2 * rows, wide), 0)
        query_row = lax.broadcasted_iota(jnp.int32, (2 * rows, wide), 1) % rows
        keys = kv[0, h, KEYS, :, :, cols].reshape(2 * rows, HEAD_SIZE)
        values = kv[0, h, VALUES, :, :, cols].reshape(2 * rows, HEAD_SIZE)
        first = unit(keys[:rows], values[:rows], g, 0, wide, key_row[:rows] <= query_row[:rows], True)
        second = unit(keys, values, g, 1, wide, key_row <= query_row + rows, True)
        for what in (KEYS, VALUES):
            part[0, h, what, 0, :, cols] = first[what] + second[what][:rows]
            part[0, h, what, 1, :, cols] = second[what][rows:]

    def own_half(h, _):
        for i in range(some):
            own_shard(h, i)
        return 0

    lax.fori_loop(0, HALVES, own_half, 0)

    def slot_of(way, step):
        return n - 1 - step if way == RIGHT else 1 + step

    def send_sums(way, step, first):
        for what in (KEYS, VALUES):
            if not first:
                for copy in sum_copies(way, step - 1, what):
                    copy.wait_recv()
            for block in range(2):
                total = part[slot_of(way, step), way, what, block]
                if not first:
                    total += decode(landed[way, step - 1, what, block], landed_scales[way, step - 1, what, block])
                coded[way, step, what, block], scales[way, step, what, block] = encode(total)
            for copy in sum_copies(way, step, what):
                copy.start()

    def near(step, first):
        for way in (RIGHT, LEFT):
            gather_copy(way, way, step + 1).wait_recv()
            gather_copy(way, way, step + 2).start()
        for way in (RIGHT, LEFT):
            shard(slot_of(way, step), way)
            send_sums(way, step, first)
        for way in (RIGHT, LEFT):
            gather_copy(way, 1 - way, step + 1).wait_recv()

            @pl.when(step + 2 < half)
            def _():
                gather_copy(way, 1 - way, step + 2).start()

        for way in (RIGHT, LEFT):
            shard(slot_of(way, step), 1 - way)

    if half > 1:
        near(0, True)

        def middle(step, _):
            near(step, False)
            return 0

        lax.fori_loop(1, half - 1, middle, 0)

    for way in (RIGHT, LEFT):
        gather_copy(way, way, half).wait_recv()
        shard(half, way)
        send_sums(way, half - 1, half == 1)

    def write(g, _):
        for a in range(2):
            turned = jnp.transpose(dqt[g, a]) * scaling
            for j in range(group):
                head = pl.ds(pl.multiple_of((g * group + j) * HEAD_SIZE, HEAD_SIZE), HEAD_SIZE)
                gq_ref[0, a, :, head] = turned[j * rows : (j + 1) * rows]
        return 0

    lax.fori_loop(0, kv_heads, write, 0)
    stores = [
        pltpu.make_async_copy(source, sink, out_sem.at[i])
        for i, (source, sink) in enumerate(((gq_ref, gq_hbm), (gk_ref, gk_hbm), (gv_ref, gv_hbm)))
    ]
    stores[0].start()

    def far(step, _):
        for way in (RIGHT, LEFT):
            send_sums(way, step, False)
        return 0

    lax.fori_loop(half, n - 1, far, 0)
    for way in (RIGHT, LEFT):
        cols = pl.ds(way * columns, columns)
        for what in (KEYS, VALUES):
            for copy in sum_copies(way, n - 2, what):
                copy.wait_recv()
            for block in range(2):
                total = part[0, way, what, block]
                total += decode(landed[way, n - 2, what, block], landed_scales[way, n - 2, what, block])
                if what == KEYS:
                    gk_ref[0, block, :, cols] = total * scaling
                else:
                    gv_ref[0, block, :, cols] = total
    for copy in stores[1:]:
        copy.start()

    def sent(step, _):
        for way in (RIGHT, LEFT):
            for what in (KEYS, VALUES):
                for copy in sum_copies(way, step, what):
                    copy.wait_send()
        return 0

    lax.fori_loop(0, n - 1, sent, 0)

    def passed(distance, _):
        for way in (RIGHT, LEFT):
            for h in range(HALVES):
                gather_copy(way, h, distance).wait_send()
        return 0

    lax.fori_loop(1, half, passed, 0)
    for way in (RIGHT, LEFT):
        gather_copy(way, way, half).wait_send()
    for copy in stores:
        copy.wait()


def finish(parts, gq_in, gk_in, gv_in, gq_hbm, gk_hbm, gv_hbm, gq_ref, gk_ref, gv_ref, in_sem, out_sem):
    rows = gq_in.shape[2] // parts
    pieces = [(gk_in, gk_ref, gk_hbm), (gv_in, gv_ref, gv_hbm)]
    for a in range(2):
        for i in range(parts):
            at = (0, a, pl.ds(i * rows, rows))
            pieces.append((gq_in.at[at], gq_ref.at[at], gq_hbm.at[at]))
    loads = [pltpu.make_async_copy(x, y, in_sem.at[i]) for i, (x, y, _) in enumerate(pieces)]
    stores = [pltpu.make_async_copy(y, z, out_sem.at[i]) for i, (_, y, z) in enumerate(pieces)]
    for copy in loads:
        copy.start()
    for load, store in zip(loads, stores):
        load.wait()
        store.start()
    for copy in stores:
        copy.wait()


def body(queries, keys, values, output, gradient, logsumexp):
    n = lax.axis_size("seq")
    rows = keys.shape[2]
    kv_heads = keys.shape[3] // HEAD_SIZE
    group = queries.shape[3] // keys.shape[3]
    wide = group * rows
    lse = logsumexp.transpose(0, 1, 3, 2)
    hbm = pl.BlockSpec(memory_space=pl.ANY)
    columns = keys.shape[3] // HALVES
    block = (2, 2, rows, columns)
    scale = (2, 2, 1, columns)
    bf16, f32 = jnp.bfloat16, jnp.float32
    flat = (kv_heads, 2, wide, HEAD_SIZE)
    turned = (kv_heads, 2, HEAD_SIZE, wide)
    line = (kv_heads, 2, 1, wide)
    scratch = [
        (queries.shape, bf16),
        (output.shape, bf16),
        (gradient.shape, bf16),
        (lse.shape, f32),
        (flat, bf16),
        (flat, bf16),
        (turned, bf16),
        (turned, bf16),
        (line, f32),
        (line, f32),
        (turned, f32),
        (queries.shape, f32),
        (keys.shape, f32),
        (values.shape, f32),
        ((n, HALVES) + block, bf16),
        ((n, HALVES) + block, f32),
        ((2, n - 1) + block, bf16),
        ((2, n - 1) + scale, f32),
        ((2, n - 1) + block, bf16),
        ((2, n - 1) + scale, f32),
    ]
    outputs = pl.pallas_call(
        functools.partial(kernel, n),
        out_shape=(
            jax.ShapeDtypeStruct(queries.shape, f32),
            jax.ShapeDtypeStruct(keys.shape, f32),
            jax.ShapeDtypeStruct(values.shape, f32),
        ),
        in_specs=[hbm] * 6,
        out_specs=(hbm, hbm, hbm),
        scratch_shapes=[pltpu.VMEM(shape, dtype) for shape, dtype in scratch]
        + [
            pltpu.SemaphoreType.DMA((4,)),
            pltpu.SemaphoreType.DMA((HALVES, 2)),
            pltpu.SemaphoreType.DMA((3,)),
            pltpu.SemaphoreType.DMA((2, n // 2, HALVES)),
            pltpu.SemaphoreType.DMA((2, n // 2, HALVES)),
            pltpu.SemaphoreType.DMA((2, n - 1, 2, 2)),
            pltpu.SemaphoreType.DMA((2, n - 1, 2, 2)),
        ],
        compiler_params=pltpu.CompilerParams(
            collective_id=0, has_side_effects=True, vmem_limit_bytes=64_000_000
        ),
    )(queries, keys, values, output, gradient, lse)
    shapes = [jax.ShapeDtypeStruct(x.shape, f32) for x in (queries, keys, values)]
    return pl.pallas_call(
        functools.partial(finish, PARTS),
        out_shape=shapes,
        in_specs=[hbm] * 3,
        out_specs=[hbm] * 3,
        scratch_shapes=[pltpu.VMEM(x.shape, f32) for x in shapes]
        + [pltpu.SemaphoreType.DMA((2 + 2 * PARTS,))] * 2,
        compiler_params=pltpu.CompilerParams(vmem_limit_bytes=64_000_000),
    )(*outputs)


def solution(mesh):
    spec = P("seq", None, "dp", None)
    return jax.shard_map(
        body, mesh=mesh, in_specs=(spec,) * 6, out_specs=(spec,) * 3, check_vma=False
    )
```

```python
import functools

import jax
import jax.numpy as jnp
from jax import lax
from jax.experimental import pallas as pl
from jax.experimental.pallas import tpu as pltpu
from jax.sharding import PartitionSpec as P

HEAD_SIZE = 128
LOG2E = 1.4426950408889634
LN2 = 0.6931471805599453
SPAN = 240.0
MESH = pl.DeviceIdType.MESH
KEYS, VALUES = 0, 1
HALVES = 2
PARTS = 4
RIGHT, LEFT = 0, 1


def ring_place(index, size):
    return jnp.where(index % 2 == 0, index // 2, size - 1 - index // 2)


def ring_index(place, size):
    return jnp.where(place < size // 2, 2 * place, 2 * (size - 1 - place) + 1)


def split_parts(values):
    high = values.astype(jnp.bfloat16)
    rest = (values - high.astype(jnp.float32)).astype(jnp.bfloat16)
    return jnp.concatenate([high, rest], axis=0)


def dot(a, b):
    return jnp.dot(a, b, preferred_element_type=jnp.float32)


def encode(values):
    scale = jnp.maximum(jnp.max(jnp.abs(values), axis=0, keepdims=True), 1e-30)
    level = values * (SPAN / scale)
    code = jnp.exp2(jnp.abs(level) - 0.5 * SPAN)
    return jnp.where(level < 0.0, -code, code).astype(jnp.bfloat16), scale


def decode(code, scale):
    code = code.astype(jnp.float32)
    size = jnp.log(jnp.abs(code)) * (scale * (1.0 / (SPAN * LN2))) + 0.5 * scale
    return jnp.where(code < 0.0, -size, size)


def kernel(
    n,
    q_hbm,
    k_hbm,
    v_hbm,
    o_hbm,
    g_hbm,
    lse_hbm,
    gq_hbm,
    gk_hbm,
    gv_hbm,
    q_ref,
    o_ref,
    g_ref,
    lse_ref,
    qs,
    gs,
    qt,
    gt,
    delta,
    lse,
    dqt,
    gq_ref,
    gk_ref,
    gv_ref,
    kv,
    part,
    coded,
    scales,
    landed,
    landed_scales,
    load_sem,
    own_sem,
    out_sem,
    ag_send,
    ag_recv,
    rs_send,
    rs_recv,
):
    rows = k_hbm.shape[2]
    kv_heads = k_hbm.shape[3] // HEAD_SIZE
    some = kv_heads // HALVES
    columns = some * HEAD_SIZE
    group = q_hbm.shape[3] // k_hbm.shape[3]
    wide = group * rows
    scaling = HEAD_SIZE ** (-0.5)
    me = lax.axis_index("seq")
    place = ring_place(me, n)
    right = ring_index(lax.rem(place + 1, n), n)
    left = ring_index(lax.rem(place + n - 1, n), n)
    target = (right, left)

    own = [
        pltpu.make_async_copy(
            source.at[0, block, :, pl.ds(h * columns, columns)], kv.at[0, h, block, what], own_sem.at[h, block, what]
        )
        for h in range(HALVES)
        for block in range(2)
        for what, source in ((KEYS, k_hbm), (VALUES, v_hbm))
    ]
    loads = [
        pltpu.make_async_copy(source, sink, load_sem.at[i])
        for i, (source, sink) in enumerate(
            ((q_hbm, q_ref), (g_hbm, g_ref), (o_hbm, o_ref), (lse_hbm, lse_ref))
        )
    ]
    for copy in own + loads:
        copy.start()

    barrier = pltpu.get_barrier_semaphore()
    for neighbour in (left, right):
        pl.semaphore_signal(barrier, inc=1, device_id={"seq": neighbour}, device_id_type=MESH)
    pl.semaphore_wait(barrier, 2)

    def owner_of(slot):
        return ring_index(lax.rem(place + slot, n), n)

    def near_side(way, owner):
        return owner % 2 == (1 if way == RIGHT else 0)

    def gather_copy(way, h, distance, block):
        arrives = n - distance if way == RIGHT else distance
        held = lax.rem(n + 1 - distance, n) if way == RIGHT else distance - 1
        which = distance - 1 if h == way else n - 2
        return pltpu.make_async_remote_copy(
            src_ref=kv.at[held, h, block],
            dst_ref=kv.at[arrives, h, block],
            send_sem=ag_send.at[way, which, block],
            recv_sem=ag_recv.at[way, which, block],
            device_id={"seq": target[way]},
            device_id_type=MESH,
        )

    def gathers(way, h, distance, sending, act):
        hop = distance - 1 if sending else distance
        owner = owner_of(lax.rem(n - hop, n) if way == RIGHT else hop)
        reach = n - 2 if h == way else 1
        act(gather_copy(way, h, distance, 0))

        @pl.when(jnp.where(near_side(way, owner), distance <= owner, reach >= n - owner))
        def _():
            act(gather_copy(way, h, distance, 1))

    def start(copy):
        copy.start()

    def wait_recv(copy):
        copy.wait_recv()

    def wait_send(copy):
        copy.wait_send()

    def sum_copies(way, step, block):
        return [
            pltpu.make_async_remote_copy(
                src_ref=source.at[way, step, block],
                dst_ref=sink.at[way, step, block],
                send_sem=rs_send.at[way, step, block, i],
                recv_sem=rs_recv.at[way, step, block, i],
                device_id={"seq": target[way]},
                device_id_type=MESH,
            )
            for i, (source, sink) in enumerate(((coded, landed), (scales, landed_scales)))
        ]

    def has_late(way, step, owner):
        return jnp.where(near_side(way, owner), owner > 0, step + 1 >= n - owner)

    for copy in own:
        copy.wait()
    for turn in range(HALVES):
        for way in (RIGHT, LEFT):
            gathers(way, way if turn == 0 else 1 - way, 1, True, start)
    for copy in loads:
        copy.wait()

    def prepare(g, _):
        for a in range(2):
            products = []
            for j in range(group):
                head = pl.ds(pl.multiple_of((g * group + j) * HEAD_SIZE, HEAD_SIZE), HEAD_SIZE)
                grad = g_ref[0, a, :, head]
                qs[g, a, pl.ds(j * rows, rows), :] = q_ref[0, a, :, head]
                gs[g, a, pl.ds(j * rows, rows), :] = grad
                products.append(grad.astype(jnp.float32) * o_ref[0, a, :, head].astype(jnp.float32))
            turned = jnp.transpose(jnp.concatenate(products, axis=0))
            delta[g, a] = jnp.sum(turned, axis=0, keepdims=True)
            qt[g, a] = jnp.transpose(qs[g, a])
            gt[g, a] = jnp.transpose(gs[g, a])
            tile = lse_ref[0, a, pl.ds(pl.multiple_of(g * group, group), group), :] * LOG2E
            lse[g, a] = jnp.concatenate([tile[j : j + 1] for j in range(group)], axis=1)
        return 0

    lax.fori_loop(0, kv_heads, prepare, 0)

    def unit(keys, values, g, a, chunk, mask=None, new=False):
        count = keys.shape[0]
        turned = jnp.transpose(keys)
        turned = jnp.concatenate([turned, turned], axis=1)
        key_part = value_part = 0.0
        for i in range(0, wide, chunk):
            lanes = slice(i, i + chunk)
            scores = dot(keys, qt[g, a, :, lanes])
            weights = jnp.exp2(scores * (scaling * LOG2E) - lse[g, a, :, lanes])
            if mask is not None:
                weights = jnp.where(mask[:, lanes], weights, 0.0)
            value_part += dot(split_parts(weights), gs[g, a, lanes, :])
            score_grad = weights * (dot(values, gt[g, a, :, lanes]) - delta[g, a, :, lanes])
            split = split_parts(score_grad)
            key_part += dot(split, qs[g, a, lanes, :])
            query_part = dot(turned, split)
            if new:
                dqt[g, a, :, lanes] = query_part
            else:
                dqt[g, a, :, lanes] += query_part
        return key_part[:count] + key_part[count:], value_part[:count] + value_part[count:]

    def later_shard(slot, h, i):
        cols = pl.ds(i * HEAD_SIZE, HEAD_SIZE)
        g = h * some + i
        keys = kv[slot, h, :, KEYS, :, cols].reshape(2 * rows, HEAD_SIZE)
        values = kv[slot, h, :, VALUES, :, cols].reshape(2 * rows, HEAD_SIZE)
        out = unit(keys, values, g, 1, wide)
        for what in (KEYS, VALUES):
            part[slot, h, :, what, :, cols] = out[what].reshape(2, rows, HEAD_SIZE)

    def earlier_shard(slot, h, i):
        cols = pl.ds(i * HEAD_SIZE, HEAD_SIZE)
        g = h * some + i
        keys = kv[slot, h, 0, KEYS, :, cols]
        values = kv[slot, h, 0, VALUES, :, cols]
        outs = [unit(keys, values, g, a, wide // 2) for a in range(2)]
        for what in (KEYS, VALUES):
            part[slot, h, 0, what, :, cols] = outs[0][what] + outs[1][what]
            part[slot, h, 1, what, :, cols] = jnp.zeros((rows, HEAD_SIZE), jnp.float32)

    def shard(slot, h):
        later = owner_of(slot) > me

        @pl.when(later)
        def _():
            for i in range(some):
                later_shard(slot, h, i)

        @pl.when(jnp.logical_not(later))
        def _():
            for i in range(some):
                earlier_shard(slot, h, i)

    def own_shard(h, i):
        cols = pl.ds(i * HEAD_SIZE, HEAD_SIZE)
        g = h * some + i
        key_row = lax.broadcasted_iota(jnp.int32, (2 * rows, wide), 0)
        query_row = lax.broadcasted_iota(jnp.int32, (2 * rows, wide), 1) % rows
        keys = kv[0, h, :, KEYS, :, cols].reshape(2 * rows, HEAD_SIZE)
        values = kv[0, h, :, VALUES, :, cols].reshape(2 * rows, HEAD_SIZE)
        first = unit(keys[:rows], values[:rows], g, 0, wide, key_row[:rows] <= query_row[:rows], True)
        second = unit(keys, values, g, 1, wide, key_row <= query_row + rows, True)
        for what in (KEYS, VALUES):
            part[0, h, 0, what, :, cols] = first[what] + second[what][:rows]
            part[0, h, 1, what, :, cols] = second[what][rows:]

    def own_half(h, _):
        for i in range(some):
            own_shard(h, i)
        return 0

    lax.fori_loop(0, HALVES, own_half, 0)

    def slot_of(way, step):
        return n - 1 - step if way == RIGHT else 1 + step

    def send_sums(way, step, first):
        slot = slot_of(way, step)
        owner = owner_of(slot)

        def pass_on(block, add):
            if add:
                for copy in sum_copies(way, step - 1, block):
                    copy.wait_recv()
            for what in (KEYS, VALUES):
                total = part[slot, way, block, what]
                if add:
                    total += decode(landed[way, step - 1, block, what], landed_scales[way, step - 1, block, what])
                coded[way, step, block, what], scales[way, step, block, what] = encode(total)
            for copy in sum_copies(way, step, block):
                copy.start()

        pass_on(0, not first)
        sends = has_late(way, step, owner)
        if first:
            pl.when(sends)(lambda: pass_on(1, False))
        else:
            adds = has_late(way, step - 1, owner)
            pl.when(adds)(lambda: pass_on(1, True))
            pl.when(jnp.logical_and(sends, jnp.logical_not(adds)))(lambda: pass_on(1, False))

    def near(step, first):
        for way in (RIGHT, LEFT):
            gathers(way, way, step + 1, False, wait_recv)

            @pl.when(step + 2 < n - 1)
            def _():
                gathers(way, way, step + 2, True, start)

        for way in (RIGHT, LEFT):
            shard(slot_of(way, step), way)
            send_sums(way, step, first)

    near(0, True)

    def middle(step, _):
        near(step, False)
        return 0

    lax.fori_loop(1, n - 2, middle, 0)
    for way in (RIGHT, LEFT):
        gathers(1 - way, way, 1, False, wait_recv)
        shard(slot_of(way, n - 2), way)
    for way in (RIGHT, LEFT):
        send_sums(way, n - 2, False)

    def write(g, _):
        for a in range(2):
            turned = jnp.transpose(dqt[g, a]) * scaling
            for j in range(group):
                head = pl.ds(pl.multiple_of((g * group + j) * HEAD_SIZE, HEAD_SIZE), HEAD_SIZE)
                gq_ref[0, a, :, head] = turned[j * rows : (j + 1) * rows]
        return 0

    lax.fori_loop(0, kv_heads, write, 0)
    stores = [
        pltpu.make_async_copy(source, sink, out_sem.at[i])
        for i, (source, sink) in enumerate(((gq_ref, gq_hbm), (gk_ref, gk_hbm), (gv_ref, gv_hbm)))
    ]
    stores[0].start()

    def sent(step):
        for way in (RIGHT, LEFT):
            for copy in sum_copies(way, step, 0):
                copy.wait_send()

            @pl.when(has_late(way, step, owner_of(slot_of(way, step))))
            def _():
                for copy in sum_copies(way, step, 1):
                    copy.wait_send()

    def passed(step, _):
        sent(step)
        for way in (RIGHT, LEFT):
            gathers(way, way, step + 1, True, wait_send)
        return 0

    lax.fori_loop(0, n - 2, passed, 0)
    for way in (RIGHT, LEFT):
        gathers(way, 1 - way, 1, True, wait_send)

    for way in (RIGHT, LEFT):
        cols = pl.ds(way * columns, columns)
        for block in range(2):

            def finish_block(add):
                if add:
                    for copy in sum_copies(way, n - 2, block):
                        copy.wait_recv()
                for what in (KEYS, VALUES):
                    total = part[0, way, block, what]
                    if add:
                        total += decode(landed[way, n - 2, block, what], landed_scales[way, n - 2, block, what])
                    if what == KEYS:
                        gk_ref[0, block, :, cols] = total * scaling
                    else:
                        gv_ref[0, block, :, cols] = total

            if block == 0:
                finish_block(True)
            else:
                pl.when(me > 0)(lambda: finish_block(True))
                pl.when(me == 0)(lambda: finish_block(False))
    for copy in stores[1:]:
        copy.start()

    sent(n - 2)
    for copy in stores:
        copy.wait()


def finish(parts, gq_in, gk_in, gv_in, gq_hbm, gk_hbm, gv_hbm, gq_ref, gk_ref, gv_ref, in_sem, out_sem):
    rows = gq_in.shape[2] // parts
    pieces = [(gk_in, gk_ref, gk_hbm), (gv_in, gv_ref, gv_hbm)]
    for a in range(2):
        for i in range(parts):
            at = (0, a, pl.ds(i * rows, rows))
            pieces.append((gq_in.at[at], gq_ref.at[at], gq_hbm.at[at]))
    loads = [pltpu.make_async_copy(x, y, in_sem.at[i]) for i, (x, y, _) in enumerate(pieces)]
    stores = [pltpu.make_async_copy(y, z, out_sem.at[i]) for i, (_, y, z) in enumerate(pieces)]
    for copy in loads:
        copy.start()
    for load, store in zip(loads, stores):
        load.wait()
        store.start()
    for copy in stores:
        copy.wait()


def body(queries, keys, values, output, gradient, logsumexp):
    n = lax.axis_size("seq")
    rows = keys.shape[2]
    kv_heads = keys.shape[3] // HEAD_SIZE
    group = queries.shape[3] // keys.shape[3]
    wide = group * rows
    lse = logsumexp.transpose(0, 1, 3, 2)
    hbm = pl.BlockSpec(memory_space=pl.ANY)
    columns = keys.shape[3] // HALVES
    block = (2, 2, rows, columns)
    scale = (2, 2, 1, columns)
    bf16, f32 = jnp.bfloat16, jnp.float32
    flat = (kv_heads, 2, wide, HEAD_SIZE)
    turned = (kv_heads, 2, HEAD_SIZE, wide)
    line = (kv_heads, 2, 1, wide)
    scratch = [
        (queries.shape, bf16),
        (output.shape, bf16),
        (gradient.shape, bf16),
        (lse.shape, f32),
        (flat, bf16),
        (flat, bf16),
        (turned, bf16),
        (turned, bf16),
        (line, f32),
        (line, f32),
        (turned, f32),
        (queries.shape, f32),
        (keys.shape, f32),
        (values.shape, f32),
        ((n, HALVES) + block, bf16),
        ((n, HALVES) + block, f32),
        ((2, n - 1) + block, bf16),
        ((2, n - 1) + scale, f32),
        ((2, n - 1) + block, bf16),
        ((2, n - 1) + scale, f32),
    ]
    outputs = pl.pallas_call(
        functools.partial(kernel, n),
        out_shape=(
            jax.ShapeDtypeStruct(queries.shape, f32),
            jax.ShapeDtypeStruct(keys.shape, f32),
            jax.ShapeDtypeStruct(values.shape, f32),
        ),
        in_specs=[hbm] * 6,
        out_specs=(hbm, hbm, hbm),
        scratch_shapes=[pltpu.VMEM(shape, dtype) for shape, dtype in scratch]
        + [
            pltpu.SemaphoreType.DMA((4,)),
            pltpu.SemaphoreType.DMA((HALVES, 2, 2)),
            pltpu.SemaphoreType.DMA((3,)),
            pltpu.SemaphoreType.DMA((2, n - 1, 2)),
            pltpu.SemaphoreType.DMA((2, n - 1, 2)),
            pltpu.SemaphoreType.DMA((2, n - 1, 2, 2)),
            pltpu.SemaphoreType.DMA((2, n - 1, 2, 2)),
        ],
        compiler_params=pltpu.CompilerParams(
            collective_id=0, has_side_effects=True, vmem_limit_bytes=64_000_000
        ),
    )(queries, keys, values, output, gradient, lse)
    shapes = [jax.ShapeDtypeStruct(x.shape, f32) for x in (queries, keys, values)]
    return pl.pallas_call(
        functools.partial(finish, PARTS),
        out_shape=shapes,
        in_specs=[hbm] * 3,
        out_specs=[hbm] * 3,
        scratch_shapes=[pltpu.VMEM(x.shape, f32) for x in shapes]
        + [pltpu.SemaphoreType.DMA((2 + 2 * PARTS,))] * 2,
        compiler_params=pltpu.CompilerParams(vmem_limit_bytes=64_000_000),
    )(*outputs)


def solution(mesh):
    spec = P("seq", None, "dp", None)
    return jax.shard_map(
        body, mesh=mesh, in_specs=(spec,) * 6, out_specs=(spec,) * 3, check_vma=False
    )
```

```python
import functools

import jax
import jax.numpy as jnp
from jax import lax
from jax.experimental import pallas as pl
from jax.experimental.pallas import tpu as pltpu
from jax.sharding import PartitionSpec as P

HEAD_SIZE = 128
LOG2E = 1.4426950408889634
LN2 = 0.6931471805599453
SPAN = 240.0
MESH = pl.DeviceIdType.MESH
KEYS, VALUES = 0, 1
HALVES = 2
PARTS = 4
RIGHT, LEFT = 0, 1


def ring_place(index, size):
    return jnp.where(index % 2 == 0, index // 2, size - 1 - index // 2)


def ring_index(place, size):
    return jnp.where(place < size // 2, 2 * place, 2 * (size - 1 - place) + 1)


def split_parts(values):
    high = values.astype(jnp.bfloat16)
    rest = (values - high.astype(jnp.float32)).astype(jnp.bfloat16)
    return jnp.concatenate([high, rest], axis=0)


def dot(a, b):
    return jnp.dot(a, b, preferred_element_type=jnp.float32)


def encode(values):
    scale = jnp.maximum(jnp.max(jnp.abs(values), axis=0, keepdims=True), 1e-30)
    level = values * (SPAN / scale)
    code = jnp.exp2(jnp.abs(level) - 0.5 * SPAN)
    return jnp.where(level < 0.0, -code, code).astype(jnp.bfloat16), scale


def decode(code, scale):
    code = code.astype(jnp.float32)
    size = jnp.log(jnp.abs(code)) * (scale * (1.0 / (SPAN * LN2))) + 0.5 * scale
    return jnp.where(code < 0.0, -size, size)


def kernel(
    n,
    q_hbm,
    k_hbm,
    v_hbm,
    o_hbm,
    g_hbm,
    lse_hbm,
    gq_hbm,
    gk_hbm,
    gv_hbm,
    q_ref,
    o_ref,
    g_ref,
    lse_ref,
    qs,
    gs,
    qt,
    gt,
    delta,
    lse,
    dqt,
    gq_ref,
    gk_ref,
    gv_ref,
    kv,
    part,
    coded,
    scales,
    landed,
    landed_scales,
    load_sem,
    own_sem,
    out_sem,
    ag_send,
    ag_recv,
    rs_send,
    rs_recv,
):
    rows = k_hbm.shape[2]
    kv_heads = k_hbm.shape[3] // HEAD_SIZE
    some = kv_heads // HALVES
    columns = some * HEAD_SIZE
    group = q_hbm.shape[3] // k_hbm.shape[3]
    wide = group * rows
    scaling = HEAD_SIZE ** (-0.5)
    me = lax.axis_index("seq")
    place = ring_place(me, n)
    right = ring_index(lax.rem(place + 1, n), n)
    left = ring_index(lax.rem(place + n - 1, n), n)
    target = (right, left)

    own = [
        pltpu.make_async_copy(
            source.at[0, block, :, pl.ds(h * columns, columns)], kv.at[0, h, block, what], own_sem.at[h, block, what]
        )
        for h in range(HALVES)
        for block in range(2)
        for what, source in ((KEYS, k_hbm), (VALUES, v_hbm))
    ]
    loads = [
        pltpu.make_async_copy(source, sink, load_sem.at[i])
        for i, (source, sink) in enumerate(
            ((q_hbm, q_ref), (g_hbm, g_ref), (o_hbm, o_ref), (lse_hbm, lse_ref))
        )
    ]
    barrier = pltpu.get_barrier_semaphore()
    for neighbour in (left, right):
        pl.semaphore_signal(barrier, inc=1, device_id={"seq": neighbour}, device_id_type=MESH)
    for copy in own + loads:
        copy.start()
    pl.semaphore_wait(barrier, 2)

    def owner_of(slot):
        return ring_index(lax.rem(place + slot, n), n)

    def near_side(way, owner):
        return owner % 2 == (1 if way == RIGHT else 0)

    def gather_copy(way, h, distance, block):
        arrives = n - distance if way == RIGHT else distance
        held = lax.rem(n + 1 - distance, n) if way == RIGHT else distance - 1
        which = distance - 1 if h == way else n - 2
        return pltpu.make_async_remote_copy(
            src_ref=kv.at[held, h, block],
            dst_ref=kv.at[arrives, h, block],
            send_sem=ag_send.at[way, lax.rem(distance - 1, 2) if h == way else 2, block],
            recv_sem=ag_recv.at[way, which, block],
            device_id={"seq": target[way]},
            device_id_type=MESH,
        )

    def gathers(way, h, distance, sending, act, blocks=(0, 1)):
        hop = distance - 1 if sending else distance
        owner = owner_of(lax.rem(n - hop, n) if way == RIGHT else hop)
        reach = n - 2 if h == way else 1
        if 0 in blocks:
            act(gather_copy(way, h, distance, 0))
        if 1 in blocks:
            needed = jnp.where(near_side(way, owner), distance <= owner, reach >= n - owner)
            pl.when(needed)(lambda: act(gather_copy(way, h, distance, 1)))

    def start(copy):
        copy.start()

    def wait_recv(copy):
        copy.wait_recv()

    def wait_send(copy):
        copy.wait_send()

    def sum_copies(way, step, block):
        return [
            pltpu.make_async_remote_copy(
                src_ref=source.at[way, step, block],
                dst_ref=sink.at[way, step, block],
                send_sem=rs_send.at[way, lax.rem(step, 2), block, i],
                recv_sem=rs_recv.at[way, step, block, i],
                device_id={"seq": target[way]},
                device_id_type=MESH,
            )
            for i, (source, sink) in enumerate(((coded, landed), (scales, landed_scales)))
        ]

    def has_late(way, step, owner):
        return jnp.where(near_side(way, owner), owner > 0, step + 1 >= n - owner)

    for copy in own:
        copy.wait()
    for turn in range(HALVES):
        for way in (RIGHT, LEFT):
            gathers(way, way if turn == 0 else 1 - way, 1, True, start)
    for copy in loads:
        copy.wait()

    def prepare(g, _):
        for a in range(2):
            products = []
            for j in range(group):
                head = pl.ds(pl.multiple_of((g * group + j) * HEAD_SIZE, HEAD_SIZE), HEAD_SIZE)
                grad = g_ref[0, a, :, head]
                qs[g, a, pl.ds(j * rows, rows), :] = q_ref[0, a, :, head]
                gs[g, a, pl.ds(j * rows, rows), :] = grad
                products.append(grad.astype(jnp.float32) * o_ref[0, a, :, head].astype(jnp.float32))
            turned = jnp.transpose(jnp.concatenate(products, axis=0))
            delta[g, a] = jnp.sum(turned, axis=0, keepdims=True)
            qt[g, a] = jnp.transpose(qs[g, a])
            gt[g, a] = jnp.transpose(gs[g, a])
            dqt[g, a] = jnp.zeros((HEAD_SIZE, wide), jnp.float32)
            tile = lse_ref[0, a, pl.ds(pl.multiple_of(g * group, group), group), :] * LOG2E
            lse[g, a] = jnp.concatenate([tile[j : j + 1] for j in range(group)], axis=1)
        return 0

    lax.fori_loop(0, kv_heads, prepare, 0)

    def unit(keys, values, g, a, chunk, mask=None):
        count = keys.shape[0]
        turned = jnp.transpose(keys)
        turned = jnp.concatenate([turned, turned], axis=1)
        key_part = value_part = 0.0
        for i in range(0, wide, chunk):
            lanes = slice(i, i + chunk)
            scores = dot(keys, qt[g, a, :, lanes])
            weights = jnp.exp2(scores * (scaling * LOG2E) - lse[g, a, :, lanes])
            if mask is not None:
                weights = jnp.where(mask[:, lanes], weights, 0.0)
            value_part += dot(split_parts(weights), gs[g, a, lanes, :])
            score_grad = weights * (dot(values, gt[g, a, :, lanes]) - delta[g, a, :, lanes])
            split = split_parts(score_grad)
            key_part += dot(split, qs[g, a, lanes, :])
            query_part = dot(turned, split)
            dqt[g, a, :, lanes] += query_part
        return key_part[:count] + key_part[count:], value_part[:count] + value_part[count:]

    def later_shard(slot, h, i):
        cols = pl.ds(i * HEAD_SIZE, HEAD_SIZE)
        g = h * some + i
        keys = kv[slot, h, :, KEYS, :, cols].reshape(2 * rows, HEAD_SIZE)
        values = kv[slot, h, :, VALUES, :, cols].reshape(2 * rows, HEAD_SIZE)
        out = unit(keys, values, g, 1, wide)
        for what in (KEYS, VALUES):
            part[slot, h, :, what, :, cols] = out[what].reshape(2, rows, HEAD_SIZE)

    def earlier_shard(slot, h, i):
        cols = pl.ds(i * HEAD_SIZE, HEAD_SIZE)
        g = h * some + i
        keys = kv[slot, h, 0, KEYS, :, cols]
        values = kv[slot, h, 0, VALUES, :, cols]
        outs = [unit(keys, values, g, a, wide // 2) for a in range(2)]
        for what in (KEYS, VALUES):
            part[slot, h, 0, what, :, cols] = outs[0][what] + outs[1][what]
            part[slot, h, 1, what, :, cols] = jnp.zeros((rows, HEAD_SIZE), jnp.float32)

    def shard(slot, h):
        later = owner_of(slot) > me

        @pl.when(later)
        def _():
            for i in range(some):
                later_shard(slot, h, i)

        @pl.when(jnp.logical_not(later))
        def _():
            for i in range(some):
                earlier_shard(slot, h, i)

    def own_shard(h, i):
        cols = pl.ds(i * HEAD_SIZE, HEAD_SIZE)
        g = h * some + i
        key_row = lax.broadcasted_iota(jnp.int32, (2 * rows, wide), 0)
        query_row = lax.broadcasted_iota(jnp.int32, (2 * rows, wide), 1) % rows
        keys = kv[0, h, :, KEYS, :, cols].reshape(2 * rows, HEAD_SIZE)
        values = kv[0, h, :, VALUES, :, cols].reshape(2 * rows, HEAD_SIZE)
        first = unit(keys[:rows], values[:rows], g, 0, wide, key_row[:rows] <= query_row[:rows])
        second = unit(keys, values, g, 1, wide, key_row <= query_row + rows)
        for what in (KEYS, VALUES):
            part[0, h, 0, what, :, cols] = first[what] + second[what][:rows]
            part[0, h, 1, what, :, cols] = second[what][rows:]

    def own_half(h):
        def one(i, _):
            own_shard(h, i)
            return 0

        lax.fori_loop(0, some, one, 0, unroll=True)

    own_half(0)

    def slot_of(way, step):
        return n - 1 - step if way == RIGHT else 1 + step

    def sent(way, step):
        def block_sent(block):
            for copy in sum_copies(way, step, block):
                copy.wait_send()

        block_sent(0)
        pl.when(has_late(way, step, owner_of(slot_of(way, step))))(lambda: block_sent(1))

    def send_sums(way, step, first):
        slot = slot_of(way, step)
        owner = owner_of(slot)

        def pass_on(block, add):
            if add:
                for copy in sum_copies(way, step - 1, block):
                    copy.wait_recv()
            for what in (KEYS, VALUES):
                total = part[slot, way, block, what]
                if add:
                    total += decode(landed[way, step - 1, block, what], landed_scales[way, step - 1, block, what])
                coded[way, step, block, what], scales[way, step, block, what] = encode(total)
            for copy in sum_copies(way, step, block):
                copy.start()

        if not first:
            pl.when(step > 1)(lambda: sent(way, step - 2))
        pass_on(0, not first)
        sends = has_late(way, step, owner)
        if first:
            pl.when(sends)(lambda: pass_on(1, False))
        else:
            adds = has_late(way, step - 1, owner)
            pl.when(adds)(lambda: pass_on(1, True))
            pl.when(jnp.logical_and(sends, jnp.logical_not(adds)))(lambda: pass_on(1, False))

    def near(step, first):
        for block in range(2):
            for way in (RIGHT, LEFT):
                gathers(way, way, step + 1, False, wait_recv, (block,))

                @pl.when(step + 2 < n - 1)
                def _():
                    if not first:
                        gathers(way, way, step, True, wait_send, (block,))
                    gathers(way, way, step + 2, True, start, (block,))

        for way in (RIGHT, LEFT):
            shard(slot_of(way, step), way)
            send_sums(way, step, first)

    near(0, True)
    own_half(1)

    def middle(step, _):
        near(step, False)
        return 0

    lax.fori_loop(1, n - 2, middle, 0)
    for way in (RIGHT, LEFT):
        gathers(1 - way, way, 1, False, wait_recv)
        shard(slot_of(way, n - 2), way)
    for way in (RIGHT, LEFT):
        send_sums(way, n - 2, False)

    def write(g, _):
        for a in range(2):
            turned = jnp.transpose(dqt[g, a]) * scaling
            for j in range(group):
                head = pl.ds(pl.multiple_of((g * group + j) * HEAD_SIZE, HEAD_SIZE), HEAD_SIZE)
                gq_ref[0, a, :, head] = turned[j * rows : (j + 1) * rows]
        return 0

    lax.fori_loop(0, kv_heads, write, 0)
    stores = [
        pltpu.make_async_copy(source, sink, out_sem.at[i])
        for i, (source, sink) in enumerate(((gq_ref, gq_hbm), (gk_ref, gk_hbm), (gv_ref, gv_hbm)))
    ]
    stores[0].start()

    for way in (RIGHT, LEFT):
        gathers(way, way, n - 3, True, wait_send)
        gathers(way, way, n - 2, True, wait_send)
        gathers(way, 1 - way, 1, True, wait_send)
        sent(way, n - 3)

    for way in (RIGHT, LEFT):
        cols = pl.ds(way * columns, columns)
        for block in range(2):

            def finish_block(add):
                if add:
                    for copy in sum_copies(way, n - 2, block):
                        copy.wait_recv()
                for what in (KEYS, VALUES):
                    total = part[0, way, block, what]
                    if add:
                        total += decode(landed[way, n - 2, block, what], landed_scales[way, n - 2, block, what])
                    if what == KEYS:
                        gk_ref[0, block, :, cols] = total * scaling
                    else:
                        gv_ref[0, block, :, cols] = total

            if block == 0:
                finish_block(True)
            else:
                pl.when(me > 0)(lambda: finish_block(True))
                pl.when(me == 0)(lambda: finish_block(False))
    for copy in stores[1:]:
        copy.start()

    for way in (RIGHT, LEFT):
        sent(way, n - 2)
    for copy in stores:
        copy.wait()


def finish(parts, gq_in, gk_in, gv_in, gq_hbm, gk_hbm, gv_hbm, gq_ref, gk_ref, gv_ref, in_sem, out_sem):
    rows = gq_in.shape[2] // parts
    pieces = [(gk_in, gk_ref, gk_hbm), (gv_in, gv_ref, gv_hbm)]
    for a in range(2):
        for i in range(parts):
            at = (0, a, pl.ds(i * rows, rows))
            pieces.append((gq_in.at[at], gq_ref.at[at], gq_hbm.at[at]))
    loads = [pltpu.make_async_copy(x, y, in_sem.at[i]) for i, (x, y, _) in enumerate(pieces)]
    stores = [pltpu.make_async_copy(y, z, out_sem.at[i]) for i, (_, y, z) in enumerate(pieces)]
    for copy in loads:
        copy.start()
    for load, store in zip(loads, stores):
        load.wait()
        store.start()
    for copy in stores:
        copy.wait()


def body(queries, keys, values, output, gradient, logsumexp):
    n = lax.axis_size("seq")
    rows = keys.shape[2]
    kv_heads = keys.shape[3] // HEAD_SIZE
    group = queries.shape[3] // keys.shape[3]
    wide = group * rows
    lse = logsumexp.transpose(0, 1, 3, 2)
    hbm = pl.BlockSpec(memory_space=pl.ANY)
    columns = keys.shape[3] // HALVES
    block = (2, 2, rows, columns)
    scale = (2, 2, 1, columns)
    bf16, f32 = jnp.bfloat16, jnp.float32
    flat = (kv_heads, 2, wide, HEAD_SIZE)
    turned = (kv_heads, 2, HEAD_SIZE, wide)
    line = (kv_heads, 2, 1, wide)
    scratch = [
        (queries.shape, bf16),
        (output.shape, bf16),
        (gradient.shape, bf16),
        (lse.shape, f32),
        (flat, bf16),
        (flat, bf16),
        (turned, bf16),
        (turned, bf16),
        (line, f32),
        (line, f32),
        (turned, f32),
        (queries.shape, f32),
        (keys.shape, f32),
        (values.shape, f32),
        ((n, HALVES) + block, bf16),
        ((n, HALVES) + block, f32),
        ((2, n - 1) + block, bf16),
        ((2, n - 1) + scale, f32),
        ((2, n - 1) + block, bf16),
        ((2, n - 1) + scale, f32),
    ]
    outputs = pl.pallas_call(
        functools.partial(kernel, n),
        out_shape=(
            jax.ShapeDtypeStruct(queries.shape, f32),
            jax.ShapeDtypeStruct(keys.shape, f32),
            jax.ShapeDtypeStruct(values.shape, f32),
        ),
        in_specs=[hbm] * 6,
        out_specs=(hbm, hbm, hbm),
        scratch_shapes=[pltpu.VMEM(shape, dtype) for shape, dtype in scratch]
        + [
            pltpu.SemaphoreType.DMA((4,)),
            pltpu.SemaphoreType.DMA((HALVES, 2, 2)),
            pltpu.SemaphoreType.DMA((3,)),
            pltpu.SemaphoreType.DMA((2, 3, 2)),
            pltpu.SemaphoreType.DMA((2, n - 1, 2)),
            pltpu.SemaphoreType.DMA((2, 2, 2, 2)),
            pltpu.SemaphoreType.DMA((2, n - 1, 2, 2)),
        ],
        compiler_params=pltpu.CompilerParams(
            collective_id=0, has_side_effects=True, vmem_limit_bytes=64_000_000
        ),
    )(queries, keys, values, output, gradient, lse)
    shapes = [jax.ShapeDtypeStruct(x.shape, f32) for x in (queries, keys, values)]
    return pl.pallas_call(
        functools.partial(finish, PARTS),
        out_shape=shapes,
        in_specs=[hbm] * 3,
        out_specs=[hbm] * 3,
        scratch_shapes=[pltpu.VMEM(x.shape, f32) for x in shapes]
        + [pltpu.SemaphoreType.DMA((2 + 2 * PARTS,))] * 2,
        compiler_params=pltpu.CompilerParams(vmem_limit_bytes=64_000_000),
    )(*outputs)


def solution(mesh):
    spec = P("seq", None, "dp", None)
    return jax.shard_map(
        body, mesh=mesh, in_specs=(spec,) * 6, out_specs=(spec,) * 3, check_vma=False
    )
```

```python
import functools

import jax
import jax.numpy as jnp
from jax import lax
from jax.experimental import pallas as pl
from jax.experimental.pallas import tpu as pltpu
from jax.sharding import PartitionSpec as P

HEAD_SIZE = 128
LOG2E = 1.4426950408889634
LN2 = 0.6931471805599453
SPAN = 240.0
MESH = pl.DeviceIdType.MESH
KEYS, VALUES = 0, 1
HALVES = 2
PARTS = 4
RIGHT, LEFT = 0, 1


def ring_place(index, size):
    return jnp.where(index % 2 == 0, index // 2, size - 1 - index // 2)


def ring_index(place, size):
    return jnp.where(place < size // 2, 2 * place, 2 * (size - 1 - place) + 1)


def split_parts(values):
    high = values.astype(jnp.bfloat16)
    rest = (values - high.astype(jnp.float32)).astype(jnp.bfloat16)
    return jnp.concatenate([high, rest], axis=0)


def dot(a, b):
    return jnp.dot(a, b, preferred_element_type=jnp.float32)


def encode(values):
    scale = jnp.maximum(jnp.max(jnp.abs(values), axis=0, keepdims=True), 1e-30)
    level = values * (SPAN / scale)
    code = jnp.exp2(jnp.abs(level) - 0.5 * SPAN)
    return jnp.where(level < 0.0, -code, code).astype(jnp.bfloat16), scale


def decode(code, scale):
    code = code.astype(jnp.float32)
    size = jnp.log(jnp.abs(code)) * (scale * (1.0 / (SPAN * LN2))) + 0.5 * scale
    return jnp.where(code < 0.0, -size, size)


def kernel(
    n,
    q_hbm,
    k_hbm,
    v_hbm,
    o_hbm,
    g_hbm,
    lse_hbm,
    gq_hbm,
    gk_hbm,
    gv_hbm,
    q_ref,
    o_ref,
    g_ref,
    lse_ref,
    qs,
    gs,
    qt,
    gt,
    delta,
    lse,
    dqt,
    gq_ref,
    gk_ref,
    gv_ref,
    kv,
    part,
    coded,
    scales,
    landed,
    landed_scales,
    load_sem,
    own_sem,
    out_sem,
    ag_send,
    ag_recv,
    rs_send,
    rs_recv,
):
    rows = k_hbm.shape[2]
    kv_heads = k_hbm.shape[3] // HEAD_SIZE
    some = kv_heads // HALVES
    columns = some * HEAD_SIZE
    group = q_hbm.shape[3] // k_hbm.shape[3]
    wide = group * rows
    scaling = HEAD_SIZE ** (-0.5)
    me = lax.axis_index("seq")
    place = ring_place(me, n)
    right = ring_index(lax.rem(place + 1, n), n)
    left = ring_index(lax.rem(place + n - 1, n), n)
    target = (right, left)

    own = {
        (h, block, what): pltpu.make_async_copy(
            source.at[0, block, :, pl.ds(h * columns, columns)], kv.at[0, h, block, what], own_sem.at[h, block, what]
        )
        for block in range(2)
        for h in range(HALVES)
        for what, source in ((KEYS, k_hbm), (VALUES, v_hbm))
    }
    loads = [
        pltpu.make_async_copy(source, sink, load_sem.at[i])
        for i, (source, sink) in enumerate(
            ((q_hbm, q_ref), (g_hbm, g_ref), (o_hbm, o_ref), (lse_hbm, lse_ref))
        )
    ]
    barrier = pltpu.get_barrier_semaphore()
    for neighbour in (left, right):
        pl.semaphore_signal(barrier, inc=1, device_id={"seq": neighbour}, device_id_type=MESH)
    for copy in own.values():
        copy.start()
    pl.semaphore_wait(barrier, 2)

    def owner_of(slot):
        return ring_index(lax.rem(place + slot, n), n)

    def near_side(way, owner):
        return owner % 2 == (1 if way == RIGHT else 0)

    def gather_copy(way, h, distance, block):
        arrives = n - distance if way == RIGHT else distance
        held = lax.rem(n + 1 - distance, n) if way == RIGHT else distance - 1
        which = distance - 1 if h == way else n - 2
        return pltpu.make_async_remote_copy(
            src_ref=kv.at[held, h, block],
            dst_ref=kv.at[arrives, h, block],
            send_sem=ag_send.at[way, lax.rem(distance - 1, 2) if h == way else 2, block],
            recv_sem=ag_recv.at[way, which, block],
            device_id={"seq": target[way]},
            device_id_type=MESH,
        )

    def gathers(way, h, distance, sending, act, blocks=(0, 1)):
        hop = distance - 1 if sending else distance
        owner = owner_of(lax.rem(n - hop, n) if way == RIGHT else hop)
        reach = n - 2 if h == way else 1
        if 0 in blocks:
            act(gather_copy(way, h, distance, 0))
        if 1 in blocks:
            needed = jnp.where(near_side(way, owner), distance <= owner, reach >= n - owner)
            pl.when(needed)(lambda: act(gather_copy(way, h, distance, 1)))

    def start(copy):
        copy.start()

    def wait_recv(copy):
        copy.wait_recv()

    def wait_send(copy):
        copy.wait_send()

    def sum_copies(way, step, block):
        return [
            pltpu.make_async_remote_copy(
                src_ref=source.at[way, step, block],
                dst_ref=sink.at[way, step, block],
                send_sem=rs_send.at[way, lax.rem(step, 2), block, i],
                recv_sem=rs_recv.at[way, step, block, i],
                device_id={"seq": target[way]},
                device_id_type=MESH,
            )
            for i, (source, sink) in enumerate(((coded, landed), (scales, landed_scales)))
        ]

    def has_late(way, step, owner):
        return jnp.where(near_side(way, owner), owner > 0, step + 1 >= n - owner)

    for block in range(2):
        for way in (RIGHT, LEFT):
            for what in (KEYS, VALUES):
                own[way, block, what].wait()
            gathers(way, way, 1, True, start, (block,))
    for copy in loads:
        copy.start()
    for way in (RIGHT, LEFT):
        gathers(way, 1 - way, 1, True, start)
    for copy in loads:
        copy.wait()

    def prepare(g, _):
        for a in range(2):
            products = []
            for j in range(group):
                head = pl.ds(pl.multiple_of((g * group + j) * HEAD_SIZE, HEAD_SIZE), HEAD_SIZE)
                grad = g_ref[0, a, :, head]
                qs[g, a, pl.ds(j * rows, rows), :] = q_ref[0, a, :, head]
                gs[g, a, pl.ds(j * rows, rows), :] = grad
                products.append(grad.astype(jnp.float32) * o_ref[0, a, :, head].astype(jnp.float32))
            turned = jnp.transpose(jnp.concatenate(products, axis=0))
            delta[g, a] = jnp.sum(turned, axis=0, keepdims=True)
            qt[g, a] = jnp.transpose(qs[g, a])
            gt[g, a] = jnp.transpose(gs[g, a])
            dqt[g, a] = jnp.zeros((HEAD_SIZE, wide), jnp.float32)
            tile = lse_ref[0, a, pl.ds(pl.multiple_of(g * group, group), group), :] * LOG2E
            lse[g, a] = jnp.concatenate([tile[j : j + 1] for j in range(group)], axis=1)
        return 0

    lax.fori_loop(0, kv_heads, prepare, 0)

    def unit(keys, values, g, a, chunk, mask=None):
        count = keys.shape[0]
        turned = jnp.transpose(keys)
        turned = jnp.concatenate([turned, turned], axis=1)
        key_part = value_part = 0.0
        for i in range(0, wide, chunk):
            lanes = slice(i, i + chunk)
            scores = dot(keys, qt[g, a, :, lanes])
            weights = jnp.exp2(scores * (scaling * LOG2E) - lse[g, a, :, lanes])
            if mask is not None:
                weights = jnp.where(mask[:, lanes], weights, 0.0)
            value_part += dot(split_parts(weights), gs[g, a, lanes, :])
            score_grad = weights * (dot(values, gt[g, a, :, lanes]) - delta[g, a, :, lanes])
            split = split_parts(score_grad)
            key_part += dot(split, qs[g, a, lanes, :])
            query_part = dot(turned, split)
            dqt[g, a, :, lanes] += query_part
        return key_part[:count] + key_part[count:], value_part[:count] + value_part[count:]

    def later_shard(slot, h, i):
        cols = pl.ds(i * HEAD_SIZE, HEAD_SIZE)
        g = h * some + i
        keys = kv[slot, h, :, KEYS, :, cols].reshape(2 * rows, HEAD_SIZE)
        values = kv[slot, h, :, VALUES, :, cols].reshape(2 * rows, HEAD_SIZE)
        out = unit(keys, values, g, 1, wide)
        for what in (KEYS, VALUES):
            part[slot, h, :, what, :, cols] = out[what].reshape(2, rows, HEAD_SIZE)

    def earlier_shard(slot, h, i):
        cols = pl.ds(i * HEAD_SIZE, HEAD_SIZE)
        g = h * some + i
        keys = kv[slot, h, 0, KEYS, :, cols]
        values = kv[slot, h, 0, VALUES, :, cols]
        outs = [unit(keys, values, g, a, wide // 2) for a in range(2)]
        for what in (KEYS, VALUES):
            part[slot, h, 0, what, :, cols] = outs[0][what] + outs[1][what]
            part[slot, h, 1, what, :, cols] = jnp.zeros((rows, HEAD_SIZE), jnp.float32)

    def shard(slot, h):
        later = owner_of(slot) > me

        @pl.when(later)
        def _():
            for i in range(some):
                later_shard(slot, h, i)

        @pl.when(jnp.logical_not(later))
        def _():
            for i in range(some):
                earlier_shard(slot, h, i)

    def own_shard(h, i):
        cols = pl.ds(i * HEAD_SIZE, HEAD_SIZE)
        g = h * some + i
        key_row = lax.broadcasted_iota(jnp.int32, (2 * rows, wide), 0)
        query_row = lax.broadcasted_iota(jnp.int32, (2 * rows, wide), 1) % rows
        keys = kv[0, h, :, KEYS, :, cols].reshape(2 * rows, HEAD_SIZE)
        values = kv[0, h, :, VALUES, :, cols].reshape(2 * rows, HEAD_SIZE)
        first = unit(keys[:rows], values[:rows], g, 0, wide, key_row[:rows] <= query_row[:rows])
        second = unit(keys, values, g, 1, wide, key_row <= query_row + rows)
        for what in (KEYS, VALUES):
            part[0, h, 0, what, :, cols] = first[what] + second[what][:rows]
            part[0, h, 1, what, :, cols] = second[what][rows:]

    def own_half(h):
        def one(i, _):
            own_shard(h, i)
            return 0

        lax.fori_loop(0, some, one, 0, unroll=True)

    own_half(0)

    def slot_of(way, step):
        return n - 1 - step if way == RIGHT else 1 + step

    def sent(way, step):
        def block_sent(block):
            for copy in sum_copies(way, step, block):
                copy.wait_send()

        block_sent(0)
        pl.when(has_late(way, step, owner_of(slot_of(way, step))))(lambda: block_sent(1))

    def send_sums(way, step, first):
        slot = slot_of(way, step)
        owner = owner_of(slot)

        def pass_on(block, add):
            if add:
                for copy in sum_copies(way, step - 1, block):
                    copy.wait_recv()
            for what in (KEYS, VALUES):
                total = part[slot, way, block, what]
                if add:
                    total += decode(landed[way, step - 1, block, what], landed_scales[way, step - 1, block, what])
                coded[way, step, block, what], scales[way, step, block, what] = encode(total)
            for copy in sum_copies(way, step, block):
                copy.start()

        if not first:
            pl.when(step > 1)(lambda: sent(way, step - 2))
        pass_on(0, not first)
        sends = has_late(way, step, owner)
        if first:
            pl.when(sends)(lambda: pass_on(1, False))
        else:
            adds = has_late(way, step - 1, owner)
            pl.when(adds)(lambda: pass_on(1, True))
            pl.when(jnp.logical_and(sends, jnp.logical_not(adds)))(lambda: pass_on(1, False))

    def near(step, first):
        for block in range(2):
            for way in (RIGHT, LEFT):
                gathers(way, way, step + 1, False, wait_recv, (block,))

                @pl.when(step + 2 < n - 1)
                def _():
                    if not first:
                        gathers(way, way, step, True, wait_send, (block,))
                    gathers(way, way, step + 2, True, start, (block,))

        for way in (RIGHT, LEFT):
            shard(slot_of(way, step), way)
            send_sums(way, step, first)

    near(0, True)
    own_half(1)

    def middle(step, _):
        near(step, False)
        return 0

    lax.fori_loop(1, n - 2, middle, 0)
    for way in (RIGHT, LEFT):
        gathers(1 - way, way, 1, False, wait_recv)
        shard(slot_of(way, n - 2), way)
    for way in (RIGHT, LEFT):
        send_sums(way, n - 2, False)

    def write(g, _):
        for a in range(2):
            turned = jnp.transpose(dqt[g, a]) * scaling
            for j in range(group):
                head = pl.ds(pl.multiple_of((g * group + j) * HEAD_SIZE, HEAD_SIZE), HEAD_SIZE)
                gq_ref[0, a, :, head] = turned[j * rows : (j + 1) * rows]
        return 0

    lax.fori_loop(0, kv_heads, write, 0)
    stores = [
        pltpu.make_async_copy(source, sink, out_sem.at[i])
        for i, (source, sink) in enumerate(
            [(gq_ref, gq_hbm)]
            + [
                (x.at[:, :, :, pl.ds(way * columns, columns)], y.at[:, :, :, pl.ds(way * columns, columns)])
                for way in (RIGHT, LEFT)
                for x, y in ((gk_ref, gk_hbm), (gv_ref, gv_hbm))
            ]
        )
    ]
    stores[0].start()

    for way in (RIGHT, LEFT):
        gathers(way, way, n - 3, True, wait_send)
        gathers(way, way, n - 2, True, wait_send)
        gathers(way, 1 - way, 1, True, wait_send)
        sent(way, n - 3)

    for way in (RIGHT, LEFT):
        cols = pl.ds(way * columns, columns)
        for block in range(2):

            def finish_block(add):
                if add:
                    for copy in sum_copies(way, n - 2, block):
                        copy.wait_recv()
                for what in (KEYS, VALUES):
                    total = part[0, way, block, what]
                    if add:
                        total += decode(landed[way, n - 2, block, what], landed_scales[way, n - 2, block, what])
                    if what == KEYS:
                        gk_ref[0, block, :, cols] = total * scaling
                    else:
                        gv_ref[0, block, :, cols] = total

            if block == 0:
                finish_block(True)
            else:
                pl.when(me > 0)(lambda: finish_block(True))
                pl.when(me == 0)(lambda: finish_block(False))
        for copy in stores[1 + 2 * way : 3 + 2 * way]:
            copy.start()

    for way in (RIGHT, LEFT):
        sent(way, n - 2)
    for copy in stores:
        copy.wait()


def finish(parts, gq_in, gk_in, gv_in, gq_hbm, gk_hbm, gv_hbm, gq_ref, gk_ref, gv_ref, in_sem, out_sem):
    rows = gq_in.shape[2] // parts
    pieces = [(gk_in, gk_ref, gk_hbm), (gv_in, gv_ref, gv_hbm)]
    for a in range(2):
        for i in range(parts):
            at = (0, a, pl.ds(i * rows, rows))
            pieces.append((gq_in.at[at], gq_ref.at[at], gq_hbm.at[at]))
    loads = [pltpu.make_async_copy(x, y, in_sem.at[i]) for i, (x, y, _) in enumerate(pieces)]
    stores = [pltpu.make_async_copy(y, z, out_sem.at[i]) for i, (_, y, z) in enumerate(pieces)]
    for copy in loads:
        copy.start()
    for load, store in zip(loads, stores):
        load.wait()
        store.start()
    for copy in stores:
        copy.wait()


def body(queries, keys, values, output, gradient, logsumexp):
    n = lax.axis_size("seq")
    rows = keys.shape[2]
    kv_heads = keys.shape[3] // HEAD_SIZE
    group = queries.shape[3] // keys.shape[3]
    wide = group * rows
    lse = logsumexp.transpose(0, 1, 3, 2)
    hbm = pl.BlockSpec(memory_space=pl.ANY)
    columns = keys.shape[3] // HALVES
    block = (2, 2, rows, columns)
    scale = (2, 2, 1, columns)
    bf16, f32 = jnp.bfloat16, jnp.float32
    flat = (kv_heads, 2, wide, HEAD_SIZE)
    turned = (kv_heads, 2, HEAD_SIZE, wide)
    line = (kv_heads, 2, 1, wide)
    scratch = [
        (queries.shape, bf16),
        (output.shape, bf16),
        (gradient.shape, bf16),
        (lse.shape, f32),
        (flat, bf16),
        (flat, bf16),
        (turned, bf16),
        (turned, bf16),
        (line, f32),
        (line, f32),
        (turned, f32),
        (queries.shape, f32),
        (keys.shape, f32),
        (values.shape, f32),
        ((n, HALVES) + block, bf16),
        ((n, HALVES) + block, f32),
        ((2, n - 1) + block, bf16),
        ((2, n - 1) + scale, f32),
        ((2, n - 1) + block, bf16),
        ((2, n - 1) + scale, f32),
    ]
    outputs = pl.pallas_call(
        functools.partial(kernel, n),
        out_shape=(
            jax.ShapeDtypeStruct(queries.shape, f32),
            jax.ShapeDtypeStruct(keys.shape, f32),
            jax.ShapeDtypeStruct(values.shape, f32),
        ),
        in_specs=[hbm] * 6,
        out_specs=(hbm, hbm, hbm),
        scratch_shapes=[pltpu.VMEM(shape, dtype) for shape, dtype in scratch]
        + [
            pltpu.SemaphoreType.DMA((4,)),
            pltpu.SemaphoreType.DMA((HALVES, 2, 2)),
            pltpu.SemaphoreType.DMA((5,)),
            pltpu.SemaphoreType.DMA((2, 3, 2)),
            pltpu.SemaphoreType.DMA((2, n - 1, 2)),
            pltpu.SemaphoreType.DMA((2, 2, 2, 2)),
            pltpu.SemaphoreType.DMA((2, n - 1, 2, 2)),
        ],
        compiler_params=pltpu.CompilerParams(
            collective_id=0, has_side_effects=True, vmem_limit_bytes=64_000_000
        ),
    )(queries, keys, values, output, gradient, lse)
    shapes = [jax.ShapeDtypeStruct(x.shape, f32) for x in (queries, keys, values)]
    return pl.pallas_call(
        functools.partial(finish, PARTS),
        out_shape=shapes,
        in_specs=[hbm] * 3,
        out_specs=[hbm] * 3,
        scratch_shapes=[pltpu.VMEM(x.shape, f32) for x in shapes]
        + [pltpu.SemaphoreType.DMA((2 + 2 * PARTS,))] * 2,
        compiler_params=pltpu.CompilerParams(vmem_limit_bytes=64_000_000),
    )(*outputs)


def solution(mesh):
    spec = P("seq", None, "dp", None)
    return jax.shard_map(
        body, mesh=mesh, in_specs=(spec,) * 6, out_specs=(spec,) * 3, check_vma=False
    )
```

```python
import functools

import jax
import jax.numpy as jnp
from jax import lax
from jax.experimental import pallas as pl
from jax.experimental.pallas import tpu as pltpu
from jax.sharding import PartitionSpec as P

HEAD_SIZE = 128
LOG2E = 1.4426950408889634
LN2 = 0.6931471805599453
SPAN = 240.0
MESH = pl.DeviceIdType.MESH
KEYS, VALUES = 0, 1
HALVES = 2
PARTS = 4
RIGHT, LEFT = 0, 1


def ring_place(index, size):
    return jnp.where(index % 2 == 0, index // 2, size - 1 - index // 2)


def ring_index(place, size):
    return jnp.where(place < size // 2, 2 * place, 2 * (size - 1 - place) + 1)


def split_parts(values):
    high = values.astype(jnp.bfloat16)
    rest = (values - high.astype(jnp.float32)).astype(jnp.bfloat16)
    return jnp.concatenate([high, rest], axis=0)


def dot(a, b):
    return jnp.dot(a, b, preferred_element_type=jnp.float32)


def encode(values):
    scale = jnp.maximum(jnp.max(jnp.abs(values), axis=0, keepdims=True), 1e-30)
    level = values * (SPAN / scale)
    code = jnp.exp2(jnp.abs(level) - 0.5 * SPAN)
    return jnp.where(level < 0.0, -code, code).astype(jnp.bfloat16), scale


def decode(code, scale):
    code = code.astype(jnp.float32)
    size = jnp.log(jnp.abs(code)) * (scale * (1.0 / (SPAN * LN2))) + 0.5 * scale
    return jnp.where(code < 0.0, -size, size)


def kernel(
    n,
    q_hbm,
    k_hbm,
    v_hbm,
    o_hbm,
    g_hbm,
    lse_hbm,
    gq_hbm,
    gk_hbm,
    gv_hbm,
    q_ref,
    o_ref,
    g_ref,
    lse_ref,
    qs,
    gs,
    qt,
    gt,
    delta,
    lse,
    dqt,
    gq_ref,
    gk_ref,
    gv_ref,
    kv,
    part,
    coded,
    scales,
    landed,
    landed_scales,
    load_sem,
    own_sem,
    out_sem,
    ag_send,
    ag_recv,
    rs_send,
    rs_recv,
):
    rows = k_hbm.shape[2]
    kv_heads = k_hbm.shape[3] // HEAD_SIZE
    some = kv_heads // HALVES
    columns = some * HEAD_SIZE
    group = q_hbm.shape[3] // k_hbm.shape[3]
    wide = group * rows
    scaling = HEAD_SIZE ** (-0.5)
    me = lax.axis_index("seq")
    place = ring_place(me, n)
    right = ring_index(lax.rem(place + 1, n), n)
    left = ring_index(lax.rem(place + n - 1, n), n)
    target = (right, left)

    own = {
        (h, block, what): pltpu.make_async_copy(
            source.at[0, block, :, pl.ds(h * columns, columns)], kv.at[0, h, block, what], own_sem.at[h, block, what]
        )
        for block in range(2)
        for h in range(HALVES)
        for what, source in ((KEYS, k_hbm), (VALUES, v_hbm))
    }
    loads = [
        pltpu.make_async_copy(source, sink, load_sem.at[i])
        for i, (source, sink) in enumerate(
            ((q_hbm, q_ref), (g_hbm, g_ref), (o_hbm, o_ref), (lse_hbm, lse_ref))
        )
    ]
    barrier = pltpu.get_barrier_semaphore()
    for neighbour in (left, right):
        pl.semaphore_signal(barrier, inc=1, device_id={"seq": neighbour}, device_id_type=MESH)
    for copy in own.values():
        copy.start()
    pl.semaphore_wait(barrier, 2)

    def owner_of(slot):
        return ring_index(lax.rem(place + slot, n), n)

    def near_side(way, owner):
        return owner % 2 == (1 if way == RIGHT else 0)

    def gather_copy(way, h, distance, block):
        arrives = n - distance if way == RIGHT else distance
        held = lax.rem(n + 1 - distance, n) if way == RIGHT else distance - 1
        which = distance - 1 if h == way else n - 2
        return pltpu.make_async_remote_copy(
            src_ref=kv.at[held, h, block],
            dst_ref=kv.at[arrives, h, block],
            send_sem=ag_send.at[way, lax.rem(distance - 1, 2) if h == way else 2, block],
            recv_sem=ag_recv.at[way, which, block],
            device_id={"seq": target[way]},
            device_id_type=MESH,
        )

    def gathers(way, h, distance, sending, act, blocks=(0, 1)):
        hop = distance - 1 if sending else distance
        owner = owner_of(lax.rem(n - hop, n) if way == RIGHT else hop)
        reach = n - 2 if h == way else 1
        if 0 in blocks:
            act(gather_copy(way, h, distance, 0))
        if 1 in blocks:
            needed = jnp.where(near_side(way, owner), distance <= owner, reach >= n - owner)
            pl.when(needed)(lambda: act(gather_copy(way, h, distance, 1)))

    def start(copy):
        copy.start()

    def wait_recv(copy):
        copy.wait_recv()

    def wait_send(copy):
        copy.wait_send()

    def sum_copies(way, step, block):
        return [
            pltpu.make_async_remote_copy(
                src_ref=source.at[way, step, block],
                dst_ref=sink.at[way, step, block],
                send_sem=rs_send.at[way, lax.rem(step, 2), block, i],
                recv_sem=rs_recv.at[way, step, block, i],
                device_id={"seq": target[way]},
                device_id_type=MESH,
            )
            for i, (source, sink) in enumerate(((coded, landed), (scales, landed_scales)))
        ]

    def has_late(way, step, owner):
        return jnp.where(near_side(way, owner), owner > 0, step + 1 >= n - owner)

    for block in range(2):
        for way in (RIGHT, LEFT):
            for what in (KEYS, VALUES):
                own[way, block, what].wait()
            gathers(way, way, 1, True, start, (block,))
    for copy in loads:
        copy.start()
    for way in (RIGHT, LEFT):
        gathers(way, 1 - way, 1, True, start)
    for copy in loads:
        copy.wait()

    def prepare(g, _):
        for a in range(2):
            products = []
            for j in range(group):
                head = pl.ds(pl.multiple_of((g * group + j) * HEAD_SIZE, HEAD_SIZE), HEAD_SIZE)
                grad = g_ref[0, a, :, head]
                qs[g, a, pl.ds(j * rows, rows), :] = q_ref[0, a, :, head]
                gs[g, a, pl.ds(j * rows, rows), :] = grad
                products.append(grad.astype(jnp.float32) * o_ref[0, a, :, head].astype(jnp.float32))
            turned = jnp.transpose(jnp.concatenate(products, axis=0))
            delta[g, a] = jnp.sum(turned, axis=0, keepdims=True)
            qt[g, a] = jnp.transpose(qs[g, a])
            gt[g, a] = jnp.transpose(gs[g, a])
            dqt[g, a] = jnp.zeros((HEAD_SIZE, wide), jnp.float32)
            tile = lse_ref[0, a, pl.ds(pl.multiple_of(g * group, group), group), :] * LOG2E
            lse[g, a] = jnp.concatenate([tile[j : j + 1] for j in range(group)], axis=1)
        return 0

    lax.fori_loop(0, kv_heads, prepare, 0)

    def unit(keys, values, g, a, chunk, mask=None):
        count = keys.shape[0]
        turned = jnp.transpose(keys)
        turned = jnp.concatenate([turned, turned], axis=1)
        key_part = value_part = 0.0
        for i in range(0, wide, chunk):
            lanes = slice(i, i + chunk)
            scores = dot(keys, qt[g, a, :, lanes])
            weights = jnp.exp2(scores * (scaling * LOG2E) - lse[g, a, :, lanes])
            if mask is not None:
                weights = jnp.where(mask[:, lanes], weights, 0.0)
            value_part += dot(split_parts(weights), gs[g, a, lanes, :])
            score_grad = weights * (dot(values, gt[g, a, :, lanes]) - delta[g, a, :, lanes])
            split = split_parts(score_grad)
            key_part += dot(split, qs[g, a, lanes, :])
            query_part = dot(turned, split)
            dqt[g, a, :, lanes] += query_part
        return key_part[:count] + key_part[count:], value_part[:count] + value_part[count:]

    def later_shard(slot, h, i):
        cols = pl.ds(i * HEAD_SIZE, HEAD_SIZE)
        g = h * some + i
        keys = kv[slot, h, :, KEYS, :, cols].reshape(2 * rows, HEAD_SIZE)
        values = kv[slot, h, :, VALUES, :, cols].reshape(2 * rows, HEAD_SIZE)
        out = unit(keys, values, g, 1, wide)
        for what in (KEYS, VALUES):
            part[slot, h, :, what, :, cols] = out[what].reshape(2, rows, HEAD_SIZE)

    def earlier_shard(slot, h, i):
        cols = pl.ds(i * HEAD_SIZE, HEAD_SIZE)
        g = h * some + i
        keys = kv[slot, h, 0, KEYS, :, cols]
        values = kv[slot, h, 0, VALUES, :, cols]
        outs = [unit(keys, values, g, a, wide // 2) for a in range(2)]
        for what in (KEYS, VALUES):
            part[slot, h, 0, what, :, cols] = outs[0][what] + outs[1][what]
            part[slot, h, 1, what, :, cols] = jnp.zeros((rows, HEAD_SIZE), jnp.float32)

    def shard(slot, h):
        later = owner_of(slot) > me

        @pl.when(later)
        def _():
            for i in range(some):
                later_shard(slot, h, i)

        @pl.when(jnp.logical_not(later))
        def _():
            for i in range(some):
                earlier_shard(slot, h, i)

    def own_shard(h, i):
        cols = pl.ds(i * HEAD_SIZE, HEAD_SIZE)
        g = h * some + i
        key_row = lax.broadcasted_iota(jnp.int32, (2 * rows, wide), 0)
        query_row = lax.broadcasted_iota(jnp.int32, (2 * rows, wide), 1) % rows
        keys = kv[0, h, :, KEYS, :, cols].reshape(2 * rows, HEAD_SIZE)
        values = kv[0, h, :, VALUES, :, cols].reshape(2 * rows, HEAD_SIZE)
        first = unit(keys[:rows], values[:rows], g, 0, wide, key_row[:rows] <= query_row[:rows])
        second = unit(keys, values, g, 1, wide, key_row <= query_row + rows)
        for what in (KEYS, VALUES):
            part[0, h, 0, what, :, cols] = first[what] + second[what][:rows]
            part[0, h, 1, what, :, cols] = second[what][rows:]

    def own_half(h):
        def one(i, _):
            own_shard(h, i)
            return 0

        lax.fori_loop(0, some, one, 0, unroll=True)

    own_half(0)

    def slot_of(way, step):
        return n - 1 - step if way == RIGHT else 1 + step

    def sent(way, step):
        def block_sent(block):
            for copy in sum_copies(way, step, block):
                copy.wait_send()

        block_sent(0)
        pl.when(has_late(way, step, owner_of(slot_of(way, step))))(lambda: block_sent(1))

    def send_sums(way, step, first, blocks=(0, 1)):
        slot = slot_of(way, step)
        owner = owner_of(slot)

        def pass_on(block, add):
            if add:
                for copy in sum_copies(way, step - 1, block):
                    copy.wait_recv()
            for what in (KEYS, VALUES):
                total = part[slot, way, block, what]
                if add:
                    total += decode(landed[way, step - 1, block, what], landed_scales[way, step - 1, block, what])
                coded[way, step, block, what], scales[way, step, block, what] = encode(total)
            for copy in sum_copies(way, step, block):
                copy.start()

        if not first and 0 in blocks:
            pl.when(step > 1)(lambda: sent(way, step - 2))
        if 0 in blocks:
            pass_on(0, not first)
        if 1 not in blocks:
            return
        sends = has_late(way, step, owner)
        if first:
            pl.when(sends)(lambda: pass_on(1, False))
        else:
            adds = has_late(way, step - 1, owner)
            pl.when(adds)(lambda: pass_on(1, True))
            pl.when(jnp.logical_and(sends, jnp.logical_not(adds)))(lambda: pass_on(1, False))

    def near(step, first):
        for block in range(2):
            for way in (RIGHT, LEFT):
                gathers(way, way, step + 1, False, wait_recv, (block,))

                @pl.when(step + 2 < n - 1)
                def _():
                    if not first:
                        gathers(way, way, step, True, wait_send, (block,))
                    gathers(way, way, step + 2, True, start, (block,))

        for way in (RIGHT, LEFT):
            shard(slot_of(way, step), way)
            send_sums(way, step, first)

    near(0, True)
    own_half(1)

    def middle(step, _):
        near(step, False)
        return 0

    lax.fori_loop(1, n - 2, middle, 0)
    for way in (RIGHT, LEFT):
        gathers(1 - way, way, 1, False, wait_recv)
        shard(slot_of(way, n - 2), way)
    for block in range(2):
        for way in (RIGHT, LEFT):
            send_sums(way, n - 2, False, (block,))

    def write(g, _):
        for a in range(2):
            turned = jnp.transpose(dqt[g, a]) * scaling
            for j in range(group):
                head = pl.ds(pl.multiple_of((g * group + j) * HEAD_SIZE, HEAD_SIZE), HEAD_SIZE)
                gq_ref[0, a, :, head] = turned[j * rows : (j + 1) * rows]
        return 0

    lax.fori_loop(0, kv_heads, write, 0)
    stores = [
        pltpu.make_async_copy(source, sink, out_sem.at[i])
        for i, (source, sink) in enumerate(
            [(gq_ref, gq_hbm)]
            + [
                (x.at[:, :, :, pl.ds(way * columns, columns)], y.at[:, :, :, pl.ds(way * columns, columns)])
                for way in (RIGHT, LEFT)
                for x, y in ((gk_ref, gk_hbm), (gv_ref, gv_hbm))
            ]
        )
    ]
    stores[0].start()

    for way in (RIGHT, LEFT):
        gathers(way, way, n - 3, True, wait_send)
        gathers(way, way, n - 2, True, wait_send)
        gathers(way, 1 - way, 1, True, wait_send)
        sent(way, n - 3)

    for way in (RIGHT, LEFT):
        cols = pl.ds(way * columns, columns)
        for block in range(2):

            def finish_block(add):
                if add:
                    for copy in sum_copies(way, n - 2, block):
                        copy.wait_recv()
                for what in (KEYS, VALUES):
                    total = part[0, way, block, what]
                    if add:
                        total += decode(landed[way, n - 2, block, what], landed_scales[way, n - 2, block, what])
                    if what == KEYS:
                        gk_ref[0, block, :, cols] = total * scaling
                    else:
                        gv_ref[0, block, :, cols] = total

            if block == 0:
                finish_block(True)
            else:
                pl.when(me > 0)(lambda: finish_block(True))
                pl.when(me == 0)(lambda: finish_block(False))
        for copy in stores[1 + 2 * way : 3 + 2 * way]:
            copy.start()

    for way in (RIGHT, LEFT):
        sent(way, n - 2)
    for copy in stores:
        copy.wait()


def finish(parts, gq_in, gk_in, gv_in, gq_hbm, gk_hbm, gv_hbm, gq_ref, gk_ref, gv_ref, in_sem, out_sem):
    rows = gq_in.shape[2] // parts
    pieces = [(gk_in, gk_ref, gk_hbm), (gv_in, gv_ref, gv_hbm)]
    for a in range(2):
        for i in range(parts):
            at = (0, a, pl.ds(i * rows, rows))
            pieces.append((gq_in.at[at], gq_ref.at[at], gq_hbm.at[at]))
    loads = [pltpu.make_async_copy(x, y, in_sem.at[i]) for i, (x, y, _) in enumerate(pieces)]
    stores = [pltpu.make_async_copy(y, z, out_sem.at[i]) for i, (_, y, z) in enumerate(pieces)]
    for copy in loads:
        copy.start()
    for load, store in zip(loads, stores):
        load.wait()
        store.start()
    for copy in stores:
        copy.wait()


def body(queries, keys, values, output, gradient, logsumexp):
    n = lax.axis_size("seq")
    rows = keys.shape[2]
    kv_heads = keys.shape[3] // HEAD_SIZE
    group = queries.shape[3] // keys.shape[3]
    wide = group * rows
    lse = logsumexp.transpose(0, 1, 3, 2)
    hbm = pl.BlockSpec(memory_space=pl.ANY)
    columns = keys.shape[3] // HALVES
    block = (2, 2, rows, columns)
    scale = (2, 2, 1, columns)
    bf16, f32 = jnp.bfloat16, jnp.float32
    flat = (kv_heads, 2, wide, HEAD_SIZE)
    turned = (kv_heads, 2, HEAD_SIZE, wide)
    line = (kv_heads, 2, 1, wide)
    scratch = [
        (queries.shape, bf16),
        (output.shape, bf16),
        (gradient.shape, bf16),
        (lse.shape, f32),
        (flat, bf16),
        (flat, bf16),
        (turned, bf16),
        (turned, bf16),
        (line, f32),
        (line, f32),
        (turned, f32),
        (queries.shape, f32),
        (keys.shape, f32),
        (values.shape, f32),
        ((n, HALVES) + block, bf16),
        ((n, HALVES) + block, f32),
        ((2, n - 1) + block, bf16),
        ((2, n - 1) + scale, f32),
        ((2, n - 1) + block, bf16),
        ((2, n - 1) + scale, f32),
    ]
    outputs = pl.pallas_call(
        functools.partial(kernel, n),
        out_shape=(
            jax.ShapeDtypeStruct(queries.shape, f32),
            jax.ShapeDtypeStruct(keys.shape, f32),
            jax.ShapeDtypeStruct(values.shape, f32),
        ),
        in_specs=[hbm] * 6,
        out_specs=(hbm, hbm, hbm),
        scratch_shapes=[pltpu.VMEM(shape, dtype) for shape, dtype in scratch]
        + [
            pltpu.SemaphoreType.DMA((4,)),
            pltpu.SemaphoreType.DMA((HALVES, 2, 2)),
            pltpu.SemaphoreType.DMA((5,)),
            pltpu.SemaphoreType.DMA((2, 3, 2)),
            pltpu.SemaphoreType.DMA((2, n - 1, 2)),
            pltpu.SemaphoreType.DMA((2, 2, 2, 2)),
            pltpu.SemaphoreType.DMA((2, n - 1, 2, 2)),
        ],
        compiler_params=pltpu.CompilerParams(
            collective_id=0, has_side_effects=True, vmem_limit_bytes=64_000_000
        ),
    )(queries, keys, values, output, gradient, lse)
    shapes = [jax.ShapeDtypeStruct(x.shape, f32) for x in (queries, keys, values)]
    return pl.pallas_call(
        functools.partial(finish, PARTS),
        out_shape=shapes,
        in_specs=[hbm] * 3,
        out_specs=[hbm] * 3,
        scratch_shapes=[pltpu.VMEM(x.shape, f32) for x in shapes]
        + [pltpu.SemaphoreType.DMA((2 + 2 * PARTS,))] * 2,
        compiler_params=pltpu.CompilerParams(vmem_limit_bytes=64_000_000),
    )(*outputs)


def solution(mesh):
    spec = P("seq", None, "dp", None)
    return jax.shard_map(
        body, mesh=mesh, in_specs=(spec,) * 6, out_specs=(spec,) * 3, check_vma=False
    )
```
